32 devices in a mesh: groups: 2 (over y), path: 4 (over z), half: 2 (over x), tile: 2 (over core).
Axes of the slice: x: 2, y: 2, z: 4, core: 2. Of those that a mesh axis runs over, the one named last changes fastest.
Arguments:
- left_prefix: bfloat16 [64, 4096], P(('groups', 'path'), ('half', 'tile')), parts along dimension 0, may hold values from -6 to 6
- right_prefix: bfloat16 [64, 4096], P(('groups', 'half', 'tile'), 'path'), parts along dimension 0, may hold values from -6 to 6
- left_layer: bfloat16 [2048, 1024], P(('groups', 'half', 'tile')), parts along dimension 0, may hold values from -0.1875 to 0.1875
- right_layer: bfloat16 [2048, 1024], P(('groups', 'path')), parts along dimension 0, may hold values from -0.1875 to 0.1875
- left_map: int32 [512], P('groups'), parts along dimension 0, may hold values from 0 to 31
- right_map: int32 [512], P('groups'), parts along dimension 0, may hold values from 0 to 31
- branch_bits: int32 [512, 10], P('groups'), parts along dimension 0, may hold values 0 or 1
- cut_side: int32 [20], P('groups'), parts along dimension 0, may hold values 0 or 1
Outputs:
- amplitude: bfloat16 [8192, 4096], P(('groups', 'half', 'tile'), 'path'), parts along dimension 0
The draws below stay inside these ranges and needn't reach their ends.
There are 2 independent parts, one for each index of `groups`. The reference program is written for one: setup_inputs(seed, part) draws one part's arguments, and reference() takes and returns one part's arrays. A program takes and returns all parts, laid end to end along the dimension named above; each array names one. Nothing has to cross between parts.
All inputs are finite; a program needn't handle non-finite values.
Results may differ from the reference program's by a relative error of at most 0.0058.
Values may be sent and summed in bfloat16 or wider, within the bound.
No kernel may reach another device: no remote copies, remote signals or barrier semaphores. Data moves between devices by JAX's collectives and lax.ppermute only.
A program may use at most 64 MiB of HBM per device.

```python
import jax
import jax.numpy as jnp
from jax import lax

CUTS = 10
GATE = 1024
OUT = 4096
PATHS = 256
PREFIX = 32


def with_ends(drawn, rng, low, high):
    place = [jax.random.randint(jax.random.fold_in(rng, axis), (), 0, length) for axis, length in enumerate(drawn.shape)]
    widest = drawn.shape.index(max(drawn.shape))
    neighbour = place[:widest] + [(place[widest] + 1) % drawn.shape[widest]] + place[widest + 1:]
    return drawn.at[tuple(place)].set(low).at[tuple(neighbour)].set(high)


def level_of(key, extent, split, smallest, high):
    factor_of = 1.0
    for dim, shards_of in split:
        draws = jax.random.uniform(jax.random.fold_in(jax.random.fold_in(key, 6), dim), (shards_of,), jnp.float32, smallest / len(split), high / len(split))
        factor_of = factor_of * jnp.repeat(jnp.exp(draws), extent[dim] // shards_of).reshape((-1,) + (1,) * (len(extent) - 1 - dim))
    return factor_of


def centred(key, dims, deviation, reach, split=(), held_as=jnp.bfloat16):
    drawn = deviation * jax.random.normal(key, dims, jnp.float32)
    if split:
        drawn = drawn * level_of(key, dims, split, -0.22, 0.18)
    return jnp.clip(drawn, -reach, reach).astype(held_as)


def setup_inputs(seed: int = 0, part: int = 0) -> dict:
    key_of = jax.random.split(jax.random.key(seed), 9)
    own_keys = jax.random.split(jax.random.fold_in(key_of[8], part), 9)
    return {
        "left_prefix": centred(own_keys[0], (PREFIX, OUT), 1.0, 6.0, ((0, 4), (1, 4))),
        "right_prefix": centred(own_keys[1], (PREFIX, OUT), 1.0, 6.0, ((0, 4), (1, 4))),
        "left_layer": centred(own_keys[2], (GATE, GATE), GATE ** -0.5, 0.1875, ((0, 4),)),
        "right_layer": centred(own_keys[3], (GATE, GATE), GATE ** -0.5, 0.1875, ((0, 4),)),
        "left_map": with_ends(jax.random.randint(own_keys[4], (PATHS,), 0, PREFIX), jax.random.fold_in(own_keys[4], 1), 0, PREFIX - 1).astype(jnp.int32),
        "right_map": with_ends(jax.random.randint(own_keys[5], (PATHS,), 0, PREFIX), jax.random.fold_in(own_keys[5], 1), 0, PREFIX - 1).astype(jnp.int32),
        "branch_bits": with_ends((jax.random.randint(own_keys[6], (PATHS, CUTS), 0, 2) < 1).astype(jnp.int32), jax.random.fold_in(own_keys[6], 1), 0, 1),
        "cut_side": with_ends((jax.random.randint(own_keys[7], (CUTS,), 0, 2) < 1).astype(jnp.int32), jax.random.fold_in(own_keys[7], 1), 0, 1),
    }


def cut_factors(branch, cut_side, gate_count, on_left):
    cut_count = cut_side.shape[0]
    bit_place = lax.broadcasted_iota(jnp.int32, (cut_count, gate_count), 0)
    gate_code = lax.broadcasted_iota(jnp.int32, (cut_count, gate_count), 1)
    bit_table = jnp.right_shift(gate_code, bit_place) & 1
    projector = cut_side if on_left else 1 - cut_side
    phased = 1 - projector
    chosen = branch * projector[None, :]
    misses = jnp.sum(chosen, axis=1, keepdims=True) + jnp.dot(projector, bit_table)[None, :] - 2 * jnp.dot(chosen, bit_table)
    parity = jnp.dot(branch * phased[None, :], bit_table)
    sign_value = 1 - 2 * (parity % 2)
    return jnp.where(misses == 0, sign_value, 0).astype(jnp.float32)


def half_states(prefix, path_map, branch, cut_side, layer_matrix, on_left):
    gate_count = layer_matrix.shape[0]
    blocks = prefix.shape[1] // gate_count
    count = path_map.shape[0]
    picked = prefix[path_map].reshape(count, blocks, gate_count)
    factor = cut_factors(branch, cut_side, gate_count, on_left)
    projected = (picked.astype(jnp.float32) * factor[:, None, :]).astype(jnp.bfloat16)
    states = jnp.dot(projected.reshape(count * blocks, gate_count), layer_matrix.T, preferred_element_type=jnp.float32)
    return states.astype(jnp.bfloat16).reshape(count, blocks * gate_count)


def reference(left_prefix, right_prefix, left_layer, right_layer, left_map, right_map, branch_bits, cut_side):
    left_states = half_states(left_prefix, left_map, branch_bits, cut_side, left_layer, True)
    right_states = half_states(right_prefix, right_map, branch_bits, cut_side, right_layer, False)
    amplitude = lax.dot_general(left_states, right_states, (((0,), (0,)), ((), ())), preferred_element_type=jnp.float32)
    return amplitude.astype(jnp.bfloat16)
```

```python
import functools

import jax
import jax.numpy as jnp
from jax import lax
from jax.experimental import pallas as pl
from jax.experimental.pallas import tpu as pltpu
from jax.sharding import PartitionSpec as P

DEVICE_AXES = ("path", "half", "tile")
CONTRACT_LAST = (((1,), (1,)), ((), ()))


def cut_factors(branch, cut_side, gate_count, on_left):
    cut_count = cut_side.shape[0]
    bit_place = lax.broadcasted_iota(jnp.int32, (cut_count, gate_count), 0)
    gate_code = lax.broadcasted_iota(jnp.int32, (cut_count, gate_count), 1)
    bit_table = jnp.right_shift(gate_code, bit_place) & 1
    projector = cut_side if on_left else 1 - cut_side
    phased = 1 - projector
    chosen = branch * projector[None, :]
    misses = (
        jnp.sum(chosen, axis=1, keepdims=True)
        + jnp.dot(projector, bit_table)[None, :]
        - 2 * jnp.dot(chosen, bit_table)
    )
    parity = jnp.dot(branch * phased[None, :], bit_table)
    sign_value = 1 - 2 * (parity % 2)
    return jnp.where(misses == 0, sign_value, 0).astype(jnp.bfloat16)


def gathered(
    left_prefix, right_prefix, left_layer, right_layer, left_map, right_map, branch_bits, cut_side
):
    def states(prefix, prefix_axes, layer, layer_axes, path_map, on_left):
        rows = lax.all_gather(prefix, prefix_axes, axis=0, tiled=True)
        factor = cut_factors(branch_bits, cut_side, rows.shape[1], on_left)
        whole_layer = lax.all_gather(layer, layer_axes, axis=0, tiled=True)
        applied = lax.dot_general(
            rows[path_map] * factor, whole_layer, CONTRACT_LAST, preferred_element_type=jnp.float32
        )
        return applied.astype(jnp.bfloat16)

    left_states = states(left_prefix, "path", left_layer, ("half", "tile"), left_map, True)
    right_states = states(right_prefix, ("half", "tile"), right_layer, "path", right_map, False)
    amplitude = lax.dot_general(
        left_states, right_states, (((0,), (0,)), ((), ())), preferred_element_type=jnp.float32
    )
    return amplitude.astype(jnp.bfloat16)


def whole_vmem(count):
    return [pl.BlockSpec(memory_space=pltpu.VMEM)] * count


def small(outs):
    return pltpu.CompilerParams(vmem_limit_bytes=outs)


def project_kernel(on_left, shard_axes, pieces, *refs):
    prefix_refs, (map_ref, branch_ref, side_ref), out_ref = refs[:-4], refs[-4:-1], refs[-1]
    cuts, paths = branch_ref.shape
    gates = out_ref.shape[0]
    shard, shards = jnp.int32(0), 1
    for axis in shard_axes:
        shard = shard * lax.axis_size(axis) + lax.axis_index(axis)
        shards *= lax.axis_size(axis)
    side = side_ref[...]
    projector = side if on_left else 1 - side
    weight = jnp.left_shift(1, lax.broadcasted_iota(jnp.int32, (cuts, 1), 0))
    branch = branch_ref[...]
    wanted = jnp.sum(branch * (projector * weight), axis=0, keepdims=True)
    phased = jnp.sum(branch * ((1 - projector) * weight), axis=0, keepdims=True)
    mask = jnp.sum(projector * weight, axis=0, keepdims=True)
    gate = lax.broadcasted_iota(jnp.int32, (gates, paths), 0)
    hit = (gate & mask) == wanted
    odd = (lax.population_count(gate & phased) & 1) == 1
    factor = jnp.where(hit, jnp.where(odd, -1.0, 1.0), 0.0)
    for block in range(2):
        rows = jnp.concatenate([r[...] for r in prefix_refs[block * pieces:][:pieces]], axis=0)
        depth = rows.shape[0] // shards
        wanted_row = map_ref[...]
        place = (lax.div(wanted_row, depth) ^ shard) * depth + lax.rem(wanted_row, depth)
        index = lax.broadcasted_iota(jnp.int32, (rows.shape[0], paths), 0)
        pick = jnp.where(index == place, 1.0, 0.0).astype(jnp.bfloat16)
        picked = lax.dot_general(
            rows, pick, (((0,), (0,)), ((), ())), preferred_element_type=jnp.float32
        )
        out_ref[:, pl.ds(block * paths, paths)] = (picked * factor).astype(jnp.bfloat16)


def project(blocks, path_map, branch_bits, cut_side, on_left, shard_axes):
    pieces = len(blocks[0])
    flat = [piece for block in blocks for piece in block]
    paths = path_map.shape[0]
    return pl.pallas_call(
        functools.partial(project_kernel, on_left, shard_axes, pieces),
        out_shape=jax.ShapeDtypeStruct((flat[0].shape[1], 2 * paths), jnp.bfloat16),
        in_specs=whole_vmem(len(flat) + 3),
        out_specs=pl.BlockSpec(memory_space=pltpu.VMEM),
        compiler_params=small(16 << 20),
    )(*flat, path_map[None, :], branch_bits.T, cut_side[:, None])


def apply_kernel(count, *refs):
    layer_refs, projected_ref, mine_ref, other_ref = refs[:count], refs[count], refs[-2], refs[-1]
    paths = mine_ref.shape[1]
    at = 0
    for layer_ref in layer_refs:
        rows = layer_ref.shape[0]
        states = jnp.dot(
            layer_ref[...], projected_ref[...], preferred_element_type=jnp.float32
        ).astype(jnp.bfloat16)
        mine_ref[pl.ds(at, rows), :] = states[:, :paths]
        other_ref[pl.ds(at, rows), :] = states[:, paths:]
        at += rows


def apply_rows(layers, projected):
    rows = sum(layer.shape[0] for layer in layers)
    shape = jax.ShapeDtypeStruct((rows, projected.shape[1] // 2), jnp.bfloat16)
    return pl.pallas_call(
        functools.partial(apply_kernel, len(layers)),
        out_shape=(shape, shape),
        in_specs=whole_vmem(len(layers) + 1),
        out_specs=(pl.BlockSpec(memory_space=pltpu.VMEM),) * 2,
        compiler_params=small(16 << 20),
    )(*layers, projected)


def amplitude_kernel(left_count, *refs):
    left_refs, right_refs = refs[:left_count], refs[left_count:-4]
    out_ref, right_ref, block_ref, sems = refs[-4:]
    path, half, tile = (lax.axis_index(axis) for axis in DEVICE_AXES)
    tiles = lax.axis_size("tile")
    spot = half * tiles + tile
    near = (0, 0, 1, 1, 0, 0, 1, 1)
    turn = (0, tiles, 0, tiles, 1, 1 + tiles, 1, 1 + tiles)
    rows = right_refs[0].shape[0] // 2
    chunk = rows * tiles * lax.axis_size("half")
    for ref, plane, spin in zip(right_refs, near, turn):
        for far in range(2):
            start = (path ^ (plane + 2 * far)) * chunk + (spot ^ spin) * rows
            right_ref[pl.ds(pl.multiple_of(start, rows), rows), :] = ref[pl.ds(far * rows, rows), :]
    right = right_ref[...]
    depth = left_refs[0].shape[0]
    copies = []
    for k, (ref, spin) in enumerate(zip(left_refs, (0, 1, tiles, 1 + tiles))):
        block_ref[k] = lax.dot_general(
            ref[...], right, CONTRACT_LAST, preferred_element_type=jnp.float32
        ).astype(jnp.bfloat16)
        start = pl.multiple_of((spot ^ spin) * depth, depth)
        copy = pltpu.make_async_copy(block_ref.at[k], out_ref.at[pl.ds(start, depth), :], sems.at[k])
        copy.start()
        copies.append(copy)
    for copy in copies:
        copy.wait()


def amplitude_of(left_pieces, right_pieces):
    depth, paths = left_pieces[0].shape
    count = len(left_pieces)
    width = sum(piece.shape[0] for piece in right_pieces)
    return pl.pallas_call(
        functools.partial(amplitude_kernel, count),
        out_shape=jax.ShapeDtypeStruct((count * depth, width), jnp.bfloat16),
        in_specs=whole_vmem(count + len(right_pieces)),
        out_specs=pl.BlockSpec(memory_space=pl.ANY),
        scratch_shapes=[
            pltpu.VMEM((width, paths), jnp.bfloat16),
            pltpu.VMEM((count, depth, width), jnp.bfloat16),
            pltpu.SemaphoreType.DMA((count,)),
        ],
        compiler_params=small(16 << 20),
    )(*left_pieces, *right_pieces)


def exchanged(
    left_prefix, right_prefix, left_layer, right_layer, left_map, right_map, branch_bits, cut_side
):
    sizes = [lax.axis_size(axis) for axis in DEVICE_AXES]

    def exchange(value, plane=0, half=0, tile=0):
        pairs = []
        for p in range(sizes[0]):
            for h in range(sizes[1]):
                for t in range(sizes[2]):
                    source = (p * sizes[1] + h) * sizes[2] + t
                    target = ((p ^ plane) * sizes[1] + (h ^ half)) * sizes[2] + (t ^ tile)
                    pairs.append((source, target))
        return lax.ppermute(value, DEVICE_AXES, pairs)

    spot = lax.axis_index("half") * sizes[2] + lax.axis_index("tile")
    share = right_layer.shape[0] // (sizes[1] * sizes[2])
    near_rows = lax.dynamic_slice_in_dim(right_layer, spot * share, share, axis=0)

    tile_prefix = exchange(right_prefix, tile=1)
    far_rows = exchange(near_rows, plane=2)
    pair = jnp.concatenate([right_prefix, tile_prefix], axis=0)
    pair_x = exchange(pair, half=1)
    pair_z = exchange(pair, plane=1)
    pair_xz = exchange(pair, plane=1, half=1)
    layer_x = exchange(left_layer, half=1)
    left_rows = jnp.concatenate(
        [left_prefix] + [exchange(left_prefix, plane=step) for step in (1, 2, 3)], axis=0
    )
    left_rows_t = exchange(left_rows, tile=1)

    right_projected = project(
        ((pair, pair_x), (pair_z, pair_xz)),
        right_map, branch_bits, cut_side, False, ("half", "tile"),
    )
    right_mine, right_near = apply_rows((near_rows, far_rows), right_projected)
    right_pieces = [
        right_mine,
        exchange(right_mine, half=1),
        exchange(right_near, plane=1),
        exchange(right_near, plane=1, half=1),
    ]
    right_pieces = right_pieces + [exchange(piece, tile=1) for piece in right_pieces]

    left_projected = project(
        ((left_rows,), (left_rows_t,)), left_map, branch_bits, cut_side, True, ("path",)
    )
    own_mine, own_other = apply_rows((left_layer,), left_projected)
    x_mine, x_other = apply_rows((layer_x,), left_projected)
    left_pieces = [own_mine, exchange(own_other, tile=1), x_mine, exchange(x_other, tile=1)]
    return amplitude_of(left_pieces, right_pieces)


def solution(mesh):
    in_specs = (
        P(("groups", "path"), ("half", "tile")),
        P(("groups", "half", "tile"), "path"),
        P(("groups", "half", "tile"), None),
        P(("groups", "path"), None),
        P("groups"),
        P("groups"),
        P("groups", None),
        P("groups"),
    )
    out_specs = P(("groups", "half", "tile"), "path")
    squares = (mesh.shape["path"], mesh.shape["half"], mesh.shape["tile"]) == (4, 2, 2)
    return jax.shard_map(
        exchanged if squares else gathered,
        mesh=mesh, in_specs=in_specs, out_specs=out_specs, check_vma=False,
    )
```

```python
import functools

import jax
import jax.numpy as jnp
from jax import lax
from jax.experimental import pallas as pl
from jax.experimental.pallas import tpu as pltpu
from jax.sharding import PartitionSpec as P


DEVICE_AXES = ("path", "half", "tile")
CONTRACT_LAST = (((1,), (1,)), ((), ()))


def cut_factors(branch, cut_side, gate_count, on_left):
    cut_count = cut_side.shape[0]
    bit_place = lax.broadcasted_iota(jnp.int32, (cut_count, gate_count), 0)
    gate_code = lax.broadcasted_iota(jnp.int32, (cut_count, gate_count), 1)
    bit_table = jnp.right_shift(gate_code, bit_place) & 1
    projector = cut_side if on_left else 1 - cut_side
    phased = 1 - projector
    chosen = branch * projector[None, :]
    misses = (
        jnp.sum(chosen, axis=1, keepdims=True)
        + jnp.dot(projector, bit_table)[None, :]
        - 2 * jnp.dot(chosen, bit_table)
    )
    parity = jnp.dot(branch * phased[None, :], bit_table)
    sign_value = 1 - 2 * (parity % 2)
    return jnp.where(misses == 0, sign_value, 0).astype(jnp.bfloat16)


def gathered(
    left_prefix, right_prefix, left_layer, right_layer, left_map, right_map, branch_bits, cut_side
):
    def states(prefix, prefix_axes, layer, layer_axes, path_map, on_left):
        rows = lax.all_gather(prefix, prefix_axes, axis=0, tiled=True)
        factor = cut_factors(branch_bits, cut_side, rows.shape[1], on_left)
        whole_layer = lax.all_gather(layer, layer_axes, axis=0, tiled=True)
        applied = lax.dot_general(
            rows[path_map] * factor, whole_layer, CONTRACT_LAST, preferred_element_type=jnp.float32
        )
        return applied.astype(jnp.bfloat16)

    left_states = states(left_prefix, "path", left_layer, ("half", "tile"), left_map, True)
    right_states = states(right_prefix, ("half", "tile"), right_layer, "path", right_map, False)
    amplitude = lax.dot_general(
        left_states, right_states, (((0,), (0,)), ((), ())), preferred_element_type=jnp.float32
    )
    return amplitude.astype(jnp.bfloat16)


def call(kernel, outs, *operands, in_space=pltpu.VMEM, scratch=(), out_space=pltpu.VMEM):
    shapes = [jax.ShapeDtypeStruct(shape, jnp.bfloat16) for shape in outs]
    spaces = [in_space] * len(operands)
    if in_space == pltpu.HBM:
        operands = [pltpu.with_memory_space_constraint(x, in_space) for x in operands]
    return pl.pallas_call(
        kernel,
        out_shape=shapes,
        in_specs=[pl.BlockSpec(memory_space=space) for space in spaces],
        out_specs=[pl.BlockSpec(memory_space=out_space)] * len(shapes),
        scratch_shapes=list(scratch),
        compiler_params=pltpu.CompilerParams(vmem_limit_bytes=16 << 20),
    )(*operands)


def spot_of():
    return lax.axis_index("half") * lax.axis_size("tile") + lax.axis_index("tile")


def stage_kernel(*refs):
    sources, (outs, held, sems) = refs[:7], (refs[7:14], refs[14:18], refs[18])
    share = outs[2].shape[0]
    start = pl.multiple_of(spot_of() * share, share)
    copies = []
    for k, source in enumerate(sources):
        if k == 2:
            source = source.at[pl.ds(start, share), :]
        target = outs[k] if k < 3 else held[k - 3]
        copies.append(pltpu.make_async_copy(source, target, sems.at[k]))
        copies[-1].start()
    for copy in copies[3:]:
        copy.wait()
    side_ref, branch_ref, left_map_ref, right_map_ref = held
    out_refs = outs[3:]
    cuts, paths = branch_ref.shape
    tiles = lax.axis_size("half") * lax.axis_size("tile")
    for on_left, map_ref, shard, shards, (factor_ref, pick_ref) in (
        (True, left_map_ref, lax.axis_index("path"), lax.axis_size("path"), out_refs[:2]),
        (False, right_map_ref, spot_of(), tiles, out_refs[2:]),
    ):
        wanted = jnp.zeros((1, paths), jnp.int32)
        phased = jnp.zeros((1, paths), jnp.int32)
        mask = jnp.int32(0)
        for cut in range(cuts):
            projector = side_ref[cut] if on_left else 1 - side_ref[cut]
            bits = branch_ref[pl.ds(cut, 1), :]
            wanted += bits * (projector << cut)
            phased += bits * ((1 - projector) << cut)
            mask += projector << cut
        gate = lax.broadcasted_iota(jnp.int32, factor_ref.shape, 0)
        hit = (gate & mask) == wanted
        odd = (lax.population_count(gate & phased) & 1) == 1
        factor = jnp.where(hit, jnp.where(odd, -1.0, 1.0), 0.0)
        factor_ref[...] = factor.astype(jnp.bfloat16)
        rows = pick_ref.shape[0]
        depth = rows // shards
        row = map_ref[...]
        place = (lax.div(row, depth) ^ shard) * depth + lax.rem(row, depth)
        index = lax.broadcasted_iota(jnp.int32, pick_ref.shape, 0)
        pick_ref[...] = jnp.where(index == place, 1.0, 0.0).astype(jnp.bfloat16)
    for copy in copies[:3]:
        copy.wait()


def pack_kernel(right_ref, right_t_ref, left_ref, left_t_ref, rows_ref, pair_ref, near_ref, far_ref):
    depth = right_ref.shape[0]
    pair = jnp.concatenate([right_ref[...], right_t_ref[...]], axis=0)
    left = jnp.concatenate([left_ref[...], left_t_ref[...]], axis=0)
    pair_ref[...] = pair
    near_ref[pl.ds(0, 2 * depth), :] = pair
    near_ref[pl.ds(2 * depth, 2 * depth), :] = left
    share = rows_ref.shape[0]
    far_ref[pl.ds(0, share), :] = rows_ref[...]
    far_ref[pl.ds(share, 2 * depth), :] = left


def project_kernel(pieces, factor_ref, pick_ref, *refs):
    prefix_refs, out_ref = refs[:-1], refs[-1]
    paths = pick_ref.shape[1]
    factor = factor_ref[...].astype(jnp.float32)
    for block, sources in enumerate(pieces):
        rows = jnp.concatenate(
            [prefix_refs[k][pl.ds(first, count), :] for k, first, count in sources], axis=0
        )
        picked = lax.dot_general(
            rows, pick_ref[...], (((0,), (0,)), ((), ())), preferred_element_type=jnp.float32
        )
        out_ref[:, pl.ds(block * paths, paths)] = (picked * factor).astype(jnp.bfloat16)


def right_own_kernel(layer_ref, projected_ref, out_ref):
    paths = out_ref.shape[1]
    out_ref[...] = jnp.dot(
        layer_ref[...], projected_ref[:, :paths], preferred_element_type=jnp.float32
    ).astype(jnp.bfloat16)


def right_far_kernel(layer_ref, far_ref, projected_ref, mine_ref, near_ref, cross_ref):
    share, paths = mine_ref.shape
    half = near_ref.shape[0] - share
    start = pl.multiple_of(lax.axis_index("tile") * half, half)
    far = jnp.dot(
        far_ref[pl.ds(0, share), :], projected_ref[...], preferred_element_type=jnp.float32
    ).astype(jnp.bfloat16)
    mine_ref[...] = far[:, :paths]
    cross_ref[...] = far[:, paths:]
    near_ref[pl.ds(half, share), :] = far[:, paths:]
    near_ref[pl.ds(0, half), :] = jnp.dot(
        layer_ref[pl.ds(start, half), :],
        projected_ref[:, paths:],
        preferred_element_type=jnp.float32,
    ).astype(jnp.bfloat16)


def left_kernel(layer_ref, projected_ref, mine_ref, other_ref):
    paths = mine_ref.shape[1]
    states = jnp.dot(
        layer_ref[...], projected_ref[...], preferred_element_type=jnp.float32
    ).astype(jnp.bfloat16)
    mine_ref[...] = states[:, :paths]
    other_ref[...] = states[:, paths:]


def amplitude_kernel(left_count, *refs):
    left_refs, right_refs = refs[:left_count], refs[left_count:-4]
    out_ref, right_ref, block_ref, sems = refs[-4:]
    own_ref, mine_ref, x_ref, z_ref, xz_ref, mine_t_ref, x_t_ref, z_t_ref, xz_t_ref = right_refs
    path, tile, spot = lax.axis_index("path"), lax.axis_index("tile"), spot_of()
    tiles = lax.axis_size("tile")
    chunk, share = own_ref.shape[0], mine_ref.shape[0]
    half = z_ref.shape[0] - share

    def place(ref, first, count, plane, offset):
        start = pl.multiple_of((path ^ plane) * chunk + offset, count)
        right_ref[pl.ds(start, count), :] = ref[pl.ds(first, count), :]

    place(own_ref, 0, chunk, 0, 0)
    place(z_ref, 0, half, 1, tile * half)
    place(z_t_ref, 0, half, 1, (tile ^ 1) * half)
    for spin, (near_ref, x_piece, z_piece, xz_piece) in enumerate(
        ((mine_ref, x_ref, z_ref, xz_ref), (mine_t_ref, x_t_ref, z_t_ref, xz_t_ref))
    ):
        place(near_ref, 0, share, 2, (spot ^ spin) * share)
        place(x_piece, 0, share, 2, (spot ^ (spin + tiles)) * share)
        place(z_piece, half, share, 3, (spot ^ spin) * share)
        place(xz_piece, 0, share, 3, (spot ^ (spin + tiles)) * share)
    right = right_ref[...]
    depth = left_refs[0].shape[0]
    copies = []
    for k, (ref, spin) in enumerate(zip(left_refs, (0, 1, tiles, 1 + tiles))):
        block_ref[k] = lax.dot_general(
            ref[...], right, CONTRACT_LAST, preferred_element_type=jnp.float32
        ).astype(jnp.bfloat16)
        start = pl.multiple_of((spot ^ spin) * depth, depth)
        copy = pltpu.make_async_copy(block_ref.at[k], out_ref.at[pl.ds(start, depth), :], sems.at[k])
        copy.start()
        copies.append(copy)
    for copy in copies:
        copy.wait()


def exchanged(
    left_prefix, right_prefix, left_layer, right_layer, left_map, right_map, branch_bits, cut_side
):
    sizes = [lax.axis_size(axis) for axis in DEVICE_AXES]

    def exchange(value, plane=0, half=0, tile=0):
        pairs = []
        for p in range(sizes[0]):
            for h in range(sizes[1]):
                for t in range(sizes[2]):
                    source = (p * sizes[1] + h) * sizes[2] + t
                    target = ((p ^ plane) * sizes[1] + (h ^ half)) * sizes[2] + (t ^ tile)
                    pairs.append((source, target))
        return lax.ppermute(value, DEVICE_AXES, pairs)

    paths = left_map.shape[0]
    depth, gates = right_prefix.shape
    chunk = right_layer.shape[0]
    spots = sizes[1] * sizes[2]
    share = chunk // spots

    right_t = exchange(right_prefix, tile=1)
    left_t = exchange(left_prefix, tile=1)
    bits = branch_bits.T
    prefix_rows = [(sizes[0] * depth, paths), (spots * depth, paths)]
    right_own, left_own, near_rows, left_factor, left_pick, right_factor, right_pick = call(
        stage_kernel,
        [
            (depth, gates), (depth, gates), (share, gates),
            (gates, paths), prefix_rows[0], (gates, paths), prefix_rows[1],
        ],
        right_prefix, left_prefix, right_layer,
        cut_side, bits, left_map[None, :], right_map[None, :],
        in_space=pltpu.HBM,
        scratch=(
            pltpu.SMEM(cut_side.shape, jnp.int32),
            pltpu.VMEM(bits.shape, jnp.int32),
            pltpu.VMEM((1, paths), jnp.int32),
            pltpu.VMEM((1, paths), jnp.int32),
            pltpu.SemaphoreType.DMA((7,)),
        ),
    )
    pair, near_pack, far_pack = call(
        pack_kernel,
        [(2 * depth, gates), (4 * depth, gates), (share + 2 * depth, gates)],
        right_own, right_t, left_own, left_t, near_rows,
    )
    pair_x = exchange(pair, half=1)
    layer_x = exchange(left_layer, half=1)
    far = exchange(far_pack, plane=2)
    pair_xz = exchange(pair, plane=1, half=1)
    near = exchange(near_pack, plane=1)
    left_far = exchange(far_pack[share:], plane=3)

    (right_projected,) = call(
        functools.partial(
            project_kernel,
            (((0, 0, 2 * depth), (1, 0, 2 * depth)), ((2, 0, 2 * depth), (3, 0, 2 * depth))),
        ),
        [(gates, 2 * paths)],
        right_factor, right_pick, pair, pair_x, near, pair_xz,
    )
    (right_near,) = call(right_own_kernel, [(chunk, paths)], right_layer, right_projected)
    mine, for_near, cross = call(
        right_far_kernel,
        [(share, paths), (chunk // sizes[2] + share, paths), (share, paths)],
        right_layer, far, right_projected,
    )
    right_pieces = [
        mine, exchange(mine, half=1), exchange(for_near, plane=1), exchange(cross, plane=1, half=1)
    ]
    right_pieces = right_pieces + [exchange(piece, tile=1) for piece in right_pieces]

    (left_projected,) = call(
        functools.partial(
            project_kernel,
            tuple(
                (
                    (0, share + k * depth, depth),
                    (1, (2 + k) * depth, depth),
                    (2, share + k * depth, depth),
                    (3, k * depth, depth),
                )
                for k in range(2)
            ),
        ),
        [(gates, 2 * paths)],
        left_factor, left_pick, far_pack, near, far, left_far,
    )
    rows = left_layer.shape[0]
    own_mine, own_other = call(left_kernel, [(rows, paths)] * 2, left_layer, left_projected)
    x_mine, x_other = call(left_kernel, [(rows, paths)] * 2, layer_x, left_projected)
    left_pieces = [own_mine, exchange(own_other, tile=1), x_mine, exchange(x_other, tile=1)]
    (amplitude,) = call(
        functools.partial(amplitude_kernel, len(left_pieces)),
        [(spots * rows, sizes[0] * chunk)],
        *left_pieces, right_near, *right_pieces,
        scratch=(
            pltpu.VMEM((sizes[0] * chunk, paths), jnp.bfloat16),
            pltpu.VMEM((len(left_pieces), rows, sizes[0] * chunk), jnp.bfloat16),
            pltpu.SemaphoreType.DMA((len(left_pieces),)),
        ),
        out_space=pl.ANY,
    )
    return amplitude


def solution(mesh):
    in_specs = (
        P(("groups", "path"), ("half", "tile")),
        P(("groups", "half", "tile"), "path"),
        P(("groups", "half", "tile"), None),
        P(("groups", "path"), None),
        P("groups"),
        P("groups"),
        P("groups", None),
        P("groups"),
    )
    out_specs = P(("groups", "half", "tile"), "path")
    squares = (mesh.shape["path"], mesh.shape["half"], mesh.shape["tile"]) == (4, 2, 2)

    def on_device(*arrays):
        return (exchanged if squares else gathered)(*arrays)

    return jax.shard_map(
        on_device, mesh=mesh, in_specs=in_specs, out_specs=out_specs, check_vma=False
    )
```

```python
import functools

import jax
import jax.numpy as jnp
from jax import lax
from jax.experimental import pallas as pl
from jax.experimental.pallas import tpu as pltpu
from jax.sharding import PartitionSpec as P


DEVICE_AXES = ("path", "half", "tile")
CONTRACT_LAST = (((1,), (1,)), ((), ()))


def cut_factors(branch, cut_side, gate_count, on_left):
    cut_count = cut_side.shape[0]
    bit_place = lax.broadcasted_iota(jnp.int32, (cut_count, gate_count), 0)
    gate_code = lax.broadcasted_iota(jnp.int32, (cut_count, gate_count), 1)
    bit_table = jnp.right_shift(gate_code, bit_place) & 1
    projector = cut_side if on_left else 1 - cut_side
    phased = 1 - projector
    chosen = branch * projector[None, :]
    misses = (
        jnp.sum(chosen, axis=1, keepdims=True)
        + jnp.dot(projector, bit_table)[None, :]
        - 2 * jnp.dot(chosen, bit_table)
    )
    parity = jnp.dot(branch * phased[None, :], bit_table)
    sign_value = 1 - 2 * (parity % 2)
    return jnp.where(misses == 0, sign_value, 0).astype(jnp.bfloat16)


def gathered(
    left_prefix, right_prefix, left_layer, right_layer, left_map, right_map, branch_bits, cut_side
):
    def states(prefix, prefix_axes, layer, layer_axes, path_map, on_left):
        rows = lax.all_gather(prefix, prefix_axes, axis=0, tiled=True)
        factor = cut_factors(branch_bits, cut_side, rows.shape[1], on_left)
        whole_layer = lax.all_gather(layer, layer_axes, axis=0, tiled=True)
        applied = lax.dot_general(
            rows[path_map] * factor, whole_layer, CONTRACT_LAST, preferred_element_type=jnp.float32
        )
        return applied.astype(jnp.bfloat16)

    left_states = states(left_prefix, "path", left_layer, ("half", "tile"), left_map, True)
    right_states = states(right_prefix, ("half", "tile"), right_layer, "path", right_map, False)
    amplitude = lax.dot_general(
        left_states, right_states, (((0,), (0,)), ((), ())), preferred_element_type=jnp.float32
    )
    return amplitude.astype(jnp.bfloat16)


def call(kernel, outs, *operands, in_space=pltpu.VMEM, scratch=(), out_space=pltpu.VMEM):
    shapes = [
        jax.ShapeDtypeStruct(out, jnp.bfloat16) if isinstance(out, tuple) else out for out in outs
    ]
    spaces = [in_space] * len(operands)
    if in_space == pltpu.HBM:
        operands = [pltpu.with_memory_space_constraint(x, in_space) for x in operands]
    return pl.pallas_call(
        kernel,
        out_shape=shapes,
        in_specs=[pl.BlockSpec(memory_space=space) for space in spaces],
        out_specs=[pl.BlockSpec(memory_space=out_space)] * len(shapes),
        scratch_shapes=list(scratch),
        compiler_params=pltpu.CompilerParams(vmem_limit_bytes=16 << 20),
    )(*operands)


def spot_of():
    return lax.axis_index("half") * lax.axis_size("tile") + lax.axis_index("tile")


def stage_kernel(
    prefix_ref, left_ref, layer_ref, side_ref, branch_ref, left_map_ref, right_map_ref,
    own_ref, far_ref, codes_ref, side, branch, left_map, right_map, sems,
):
    depth = prefix_ref.shape[0]
    share = far_ref.shape[0] - depth
    start = pl.multiple_of(spot_of() * share, share)
    copies = [
        pltpu.make_async_copy(source, target, sems.at[k])
        for k, (source, target) in enumerate(
            (
                (side_ref, side), (branch_ref, branch),
                (left_map_ref, left_map), (right_map_ref, right_map),
                (layer_ref.at[pl.ds(start, share), :], far_ref.at[pl.ds(0, share), :]),
                (left_ref, far_ref.at[pl.ds(share, depth), :]),
                (prefix_ref, own_ref),
            )
        )
    ]
    for copy in copies:
        copy.start()
    for copy in copies[:4]:
        copy.wait()
    cuts, paths = branch.shape
    for half, (map_ref, shard) in enumerate(
        ((left_map, lax.axis_index("path")), (right_map, spot_of()))
    ):
        wanted = jnp.zeros((1, paths), jnp.int32)
        phased = jnp.zeros((1, paths), jnp.int32)
        mask = jnp.int32(0)
        for cut in range(cuts):
            projector = 1 - side[cut] if half else side[cut]
            bits = branch[pl.ds(cut, 1), :]
            wanted += bits * (projector << cut)
            phased += bits * ((1 - projector) << cut)
            mask += projector << cut
        row = map_ref[...]
        place = (lax.div(row, depth) ^ shard) * depth + lax.rem(row, depth)
        for k, code in enumerate((wanted, phased, place, jnp.full((1, paths), mask))):
            codes_ref[pl.ds(4 * half + k, 1), :] = code
    for copy in copies[4:]:
        copy.wait()


def mask_kernel(codes_ref, *out_refs):
    for half in range(2):
        factor_ref, pick_ref = out_refs[2 * half:][:2]
        wanted, phased, place, mask = (codes_ref[pl.ds(4 * half + k, 1), :] for k in range(4))
        gate = lax.broadcasted_iota(jnp.int32, factor_ref.shape, 0)
        hit = (gate & mask) == wanted
        odd = (lax.population_count(gate & phased) & 1) == 1
        factor = jnp.where(hit, jnp.where(odd, -1.0, 1.0), 0.0)
        factor_ref[...] = factor.astype(jnp.bfloat16)
        index = lax.broadcasted_iota(jnp.int32, pick_ref.shape, 0)
        pick_ref[...] = jnp.where(index == place, 1.0, 0.0).astype(jnp.bfloat16)


def pack_kernel(own_ref, own_t_ref, far_ref, pair_ref, near_ref):
    depth = own_ref.shape[0]
    pair = jnp.concatenate([own_ref[...], own_t_ref[...]], axis=0)
    pair_ref[...] = pair
    near_ref[pl.ds(0, 2 * depth), :] = pair
    near_ref[pl.ds(2 * depth, depth), :] = far_ref[pl.ds(far_ref.shape[0] - depth, depth), :]


def left_pack_kernel(own_ref, near_ref, far_ref, cross_ref, out_ref):
    depth = cross_ref.shape[0]
    for k, ref in enumerate((own_ref, near_ref, far_ref, cross_ref)):
        out_ref[pl.ds(k * depth, depth), :] = ref[pl.ds(ref.shape[0] - depth, depth), :]


def project_kernel(pieces, factor_ref, pick_ref, *refs):
    prefix_refs, out_ref = refs[:-1], refs[-1]
    paths = pick_ref.shape[1]
    factor = factor_ref[...].astype(jnp.float32)
    for block, sources in enumerate(pieces):
        rows = jnp.concatenate(
            [prefix_refs[k][pl.ds(first, count), :] for k, first, count in sources], axis=0
        )
        picked = lax.dot_general(
            rows, pick_ref[...], (((0,), (0,)), ((), ())), preferred_element_type=jnp.float32
        )
        out_ref[:, pl.ds(block * paths, paths)] = (picked * factor).astype(jnp.bfloat16)


def right_own_kernel(layer_ref, projected_ref, out_ref):
    paths = out_ref.shape[1]
    out_ref[...] = jnp.dot(
        layer_ref[...], projected_ref[:, :paths], preferred_element_type=jnp.float32
    ).astype(jnp.bfloat16)


def right_far_kernel(layer_ref, far_ref, projected_ref, mine_ref, near_ref, cross_ref):
    share, paths = mine_ref.shape
    half = near_ref.shape[0] - share
    start = pl.multiple_of(lax.axis_index("tile") * half, half)
    far = jnp.dot(
        far_ref[pl.ds(0, share), :], projected_ref[...], preferred_element_type=jnp.float32
    ).astype(jnp.bfloat16)
    mine_ref[...] = far[:, :paths]
    cross_ref[...] = far[:, paths:]
    near_ref[pl.ds(half, share), :] = far[:, paths:]
    near_ref[pl.ds(0, half), :] = jnp.dot(
        layer_ref[pl.ds(start, half), :],
        projected_ref[:, paths:],
        preferred_element_type=jnp.float32,
    ).astype(jnp.bfloat16)


def left_kernel(layer_ref, projected_ref, mine_ref, other_ref):
    paths = mine_ref.shape[1]
    states = jnp.dot(
        layer_ref[...], projected_ref[...], preferred_element_type=jnp.float32
    ).astype(jnp.bfloat16)
    mine_ref[...] = states[:, :paths]
    other_ref[...] = states[:, paths:]


def amplitude_kernel(left_count, *refs):
    left_refs, right_refs = refs[:left_count], refs[left_count:-4]
    out_ref, right_ref, block_ref, sems = refs[-4:]
    own_ref, mine_ref, x_ref, z_ref, xz_ref, mine_t_ref, x_t_ref, z_t_ref, xz_t_ref = right_refs
    path, tile, spot = lax.axis_index("path"), lax.axis_index("tile"), spot_of()
    tiles = lax.axis_size("tile")
    chunk, share = own_ref.shape[0], mine_ref.shape[0]
    half = z_ref.shape[0] - share

    def place(ref, first, count, plane, offset):
        start = pl.multiple_of((path ^ plane) * chunk + offset, count)
        right_ref[pl.ds(start, count), :] = ref[pl.ds(first, count), :]

    place(own_ref, 0, chunk, 0, 0)
    place(z_ref, 0, half, 1, tile * half)
    place(z_t_ref, 0, half, 1, (tile ^ 1) * half)
    for spin, (near_ref, x_piece, z_piece, xz_piece) in enumerate(
        ((mine_ref, x_ref, z_ref, xz_ref), (mine_t_ref, x_t_ref, z_t_ref, xz_t_ref))
    ):
        place(near_ref, 0, share, 2, (spot ^ spin) * share)
        place(x_piece, 0, share, 2, (spot ^ (spin + tiles)) * share)
        place(z_piece, half, share, 3, (spot ^ spin) * share)
        place(xz_piece, 0, share, 3, (spot ^ (spin + tiles)) * share)
    right = right_ref[...]
    depth = left_refs[0].shape[0]
    copies = []
    for k, (ref, spin) in enumerate(zip(left_refs, (0, 1, tiles, 1 + tiles))):
        block_ref[k] = lax.dot_general(
            ref[...], right, CONTRACT_LAST, preferred_element_type=jnp.float32
        ).astype(jnp.bfloat16)
        start = pl.multiple_of((spot ^ spin) * depth, depth)
        copy = pltpu.make_async_copy(block_ref.at[k], out_ref.at[pl.ds(start, depth), :], sems.at[k])
        copy.start()
        copies.append(copy)
    for copy in copies:
        copy.wait()


def exchanged(
    left_prefix, right_prefix, left_layer, right_layer, left_map, right_map, branch_bits, cut_side
):
    sizes = [lax.axis_size(axis) for axis in DEVICE_AXES]

    def exchange(value, plane=0, half=0, tile=0):
        pairs = []
        for p in range(sizes[0]):
            for h in range(sizes[1]):
                for t in range(sizes[2]):
                    source = (p * sizes[1] + h) * sizes[2] + t
                    target = ((p ^ plane) * sizes[1] + (h ^ half)) * sizes[2] + (t ^ tile)
                    pairs.append((source, target))
        return lax.ppermute(value, DEVICE_AXES, pairs)

    paths = left_map.shape[0]
    depth, gates = right_prefix.shape
    chunk = right_layer.shape[0]
    spots = sizes[1] * sizes[2]
    share = chunk // spots

    bits = branch_bits.T
    own, far_pack, codes = call(
        stage_kernel,
        [(depth, gates), (share + depth, gates), jax.ShapeDtypeStruct((8, paths), jnp.int32)],
        right_prefix, left_prefix, right_layer,
        cut_side, bits, left_map[None, :], right_map[None, :],
        in_space=pltpu.HBM,
        scratch=(
            pltpu.SMEM(cut_side.shape, jnp.int32),
            pltpu.VMEM(bits.shape, jnp.int32),
            pltpu.VMEM((1, paths), jnp.int32),
            pltpu.VMEM((1, paths), jnp.int32),
            pltpu.SemaphoreType.DMA((7,)),
        ),
    )
    far = exchange(far_pack, plane=2)
    prefix_x = exchange(right_prefix, half=1)
    layer_x = exchange(left_layer, half=1)
    own_t = exchange(own, tile=1)
    left_factor, left_pick, right_factor, right_pick = call(
        mask_kernel,
        [(gates, paths), (sizes[0] * depth, paths), (gates, paths), (spots * depth, paths)],
        codes,
    )
    pair, near_pack = call(
        pack_kernel, [(2 * depth, gates), (3 * depth, gates)], own, own_t, far_pack
    )
    near = exchange(near_pack, plane=1)
    pair_xz = exchange(pair, plane=1, half=1)
    left_cross = exchange(left_prefix, plane=3)
    prefix_xt = exchange(prefix_x, tile=1)

    (right_projected,) = call(
        functools.partial(
            project_kernel,
            (
                ((0, 0, 2 * depth), (1, 0, depth), (2, 0, depth)),
                ((3, 0, 2 * depth), (4, 0, 2 * depth)),
            ),
        ),
        [(gates, 2 * paths)],
        right_factor, right_pick, pair, prefix_x, prefix_xt, near, pair_xz,
    )
    mine, for_near, cross = call(
        right_far_kernel,
        [(share, paths), (chunk // sizes[2] + share, paths), (share, paths)],
        right_layer, far, right_projected,
    )
    right_pieces = [
        mine, exchange(mine, half=1), exchange(for_near, plane=1), exchange(cross, plane=1, half=1)
    ]
    right_pieces = right_pieces + [exchange(piece, tile=1) for piece in right_pieces]
    (right_near,) = call(right_own_kernel, [(chunk, paths)], right_layer, right_projected)

    (left_rows,) = call(
        left_pack_kernel, [(sizes[0] * depth, gates)], far_pack, near, far, left_cross
    )
    left_rows_t = exchange(left_rows, tile=1)
    (left_projected,) = call(
        functools.partial(
            project_kernel, tuple(((k, 0, sizes[0] * depth),) for k in range(2))
        ),
        [(gates, 2 * paths)],
        left_factor, left_pick, left_rows, left_rows_t,
    )
    rows = left_layer.shape[0]
    own_mine, own_other = call(left_kernel, [(rows, paths)] * 2, left_layer, left_projected)
    x_mine, x_other = call(left_kernel, [(rows, paths)] * 2, layer_x, left_projected)
    left_pieces = [own_mine, exchange(own_other, tile=1), x_mine, exchange(x_other, tile=1)]
    (amplitude,) = call(
        functools.partial(amplitude_kernel, len(left_pieces)),
        [(spots * rows, sizes[0] * chunk)],
        *left_pieces, right_near, *right_pieces,
        scratch=(
            pltpu.VMEM((sizes[0] * chunk, paths), jnp.bfloat16),
            pltpu.VMEM((len(left_pieces), rows, sizes[0] * chunk), jnp.bfloat16),
            pltpu.SemaphoreType.DMA((len(left_pieces),)),
        ),
        out_space=pl.ANY,
    )
    return amplitude


def solution(mesh):
    in_specs = (
        P(("groups", "path"), ("half", "tile")),
        P(("groups", "half", "tile"), "path"),
        P(("groups", "half", "tile"), None),
        P(("groups", "path"), None),
        P("groups"),
        P("groups"),
        P("groups", None),
        P("groups"),
    )
    out_specs = P(("groups", "half", "tile"), "path")
    squares = (mesh.shape["path"], mesh.shape["half"], mesh.shape["tile"]) == (4, 2, 2)

    def on_device(*arrays):
        return (exchanged if squares else gathered)(*arrays)

    return jax.shard_map(
        on_device, mesh=mesh, in_specs=in_specs, out_specs=out_specs, check_vma=False
    )
```

```python
import functools

import jax
import jax.numpy as jnp
from jax import lax
from jax.experimental import pallas as pl
from jax.experimental.pallas import tpu as pltpu
from jax.sharding import PartitionSpec as P


DEVICE_AXES = ("path", "half", "tile")
CONTRACT_LAST = (((1,), (1,)), ((), ()))


def cut_factors(branch, cut_side, gate_count, on_left):
    cut_count = cut_side.shape[0]
    bit_place = lax.broadcasted_iota(jnp.int32, (cut_count, gate_count), 0)
    gate_code = lax.broadcasted_iota(jnp.int32, (cut_count, gate_count), 1)
    bit_table = jnp.right_shift(gate_code, bit_place) & 1
    projector = cut_side if on_left else 1 - cut_side
    phased = 1 - projector
    chosen = branch * projector[None, :]
    misses = (
        jnp.sum(chosen, axis=1, keepdims=True)
        + jnp.dot(projector, bit_table)[None, :]
        - 2 * jnp.dot(chosen, bit_table)
    )
    parity = jnp.dot(branch * phased[None, :], bit_table)
    sign_value = 1 - 2 * (parity % 2)
    return jnp.where(misses == 0, sign_value, 0).astype(jnp.bfloat16)


def gathered(
    left_prefix, right_prefix, left_layer, right_layer, left_map, right_map, branch_bits, cut_side
):
    def states(prefix, prefix_axes, layer, layer_axes, path_map, on_left):
        rows = lax.all_gather(prefix, prefix_axes, axis=0, tiled=True)
        factor = cut_factors(branch_bits, cut_side, rows.shape[1], on_left)
        whole_layer = lax.all_gather(layer, layer_axes, axis=0, tiled=True)
        applied = lax.dot_general(
            rows[path_map] * factor, whole_layer, CONTRACT_LAST, preferred_element_type=jnp.float32
        )
        return applied.astype(jnp.bfloat16)

    left_states = states(left_prefix, "path", left_layer, ("half", "tile"), left_map, True)
    right_states = states(right_prefix, ("half", "tile"), right_layer, "path", right_map, False)
    amplitude = lax.dot_general(
        left_states, right_states, (((0,), (0,)), ((), ())), preferred_element_type=jnp.float32
    )
    return amplitude.astype(jnp.bfloat16)


def call(kernel, outs, *operands, in_space=pltpu.VMEM, scratch=(), out_space=pltpu.VMEM):
    shapes = [
        jax.ShapeDtypeStruct(out, jnp.bfloat16) if isinstance(out, tuple) else out for out in outs
    ]
    spaces = [in_space] * len(operands)
    if in_space == pltpu.HBM:
        operands = [pltpu.with_memory_space_constraint(x, in_space) for x in operands]
    return pl.pallas_call(
        kernel,
        out_shape=shapes,
        in_specs=[pl.BlockSpec(memory_space=space) for space in spaces],
        out_specs=[pl.BlockSpec(memory_space=out_space)] * len(shapes),
        scratch_shapes=list(scratch),
        compiler_params=pltpu.CompilerParams(vmem_limit_bytes=16 << 20),
    )(*operands)


def spot_of():
    return lax.axis_index("half") * lax.axis_size("tile") + lax.axis_index("tile")


def stage_kernel(
    prefix_ref, left_ref, layer_ref, side_ref, branch_ref, left_map_ref, right_map_ref,
    own_ref, left_own_ref, far_ref, codes_ref, side, branch, left_map, right_map, sems,
):
    depth, share = prefix_ref.shape[0], far_ref.shape[0]
    start = pl.multiple_of(spot_of() * share, share)
    copies = [
        pltpu.make_async_copy(source, target, sems.at[k])
        for k, (source, target) in enumerate(
            (
                (side_ref, side), (branch_ref, branch),
                (left_map_ref, left_map), (right_map_ref, right_map),
                (layer_ref.at[pl.ds(start, share), :], far_ref),
                (left_ref, left_own_ref),
                (prefix_ref, own_ref),
            )
        )
    ]
    for copy in copies:
        copy.start()
    for copy in copies[:4]:
        copy.wait()
    cuts, paths = branch.shape
    for half, (map_ref, shard) in enumerate(
        ((left_map, lax.axis_index("path")), (right_map, spot_of()))
    ):
        wanted = jnp.zeros((1, paths), jnp.int32)
        phased = jnp.zeros((1, paths), jnp.int32)
        mask = jnp.int32(0)
        for cut in range(cuts):
            projector = 1 - side[cut] if half else side[cut]
            bits = branch[pl.ds(cut, 1), :]
            wanted += bits * (projector << cut)
            phased += bits * ((1 - projector) << cut)
            mask += projector << cut
        row = map_ref[...]
        place = (lax.div(row, depth) ^ shard) * depth + lax.rem(row, depth)
        for k, code in enumerate((wanted, phased, place, jnp.full((1, paths), mask))):
            codes_ref[pl.ds(4 * half + k, 1), :] = code
    for copy in copies[4:]:
        copy.wait()


def mask_kernel(codes_ref, *out_refs):
    for half in range(2):
        factor_ref, pick_ref = out_refs[2 * half:][:2]
        wanted, phased, place, mask = (codes_ref[pl.ds(4 * half + k, 1), :] for k in range(4))
        gate = lax.broadcasted_iota(jnp.int32, factor_ref.shape, 0)
        hit = (gate & mask) == wanted
        odd = (lax.population_count(gate & phased) & 1) == 1
        factor = jnp.where(hit, jnp.where(odd, -1.0, 1.0), 0.0)
        factor_ref[...] = factor.astype(jnp.bfloat16)
        index = lax.broadcasted_iota(jnp.int32, pick_ref.shape, 0)
        pick_ref[...] = jnp.where(index == place, 1.0, 0.0).astype(jnp.bfloat16)


def join_kernel(sources, *refs):
    out_ref, at = refs[-1], 0
    for k, first, count in sources:
        out_ref[pl.ds(at, count), :] = refs[k][pl.ds(first, count), :]
        at += count


def project_kernel(pieces, factor_ref, pick_ref, *refs):
    prefix_refs, out_ref = refs[:-1], refs[-1]
    paths = pick_ref.shape[1]
    factor = factor_ref[...].astype(jnp.float32)
    for block, sources in enumerate(pieces):
        rows = jnp.concatenate(
            [prefix_refs[k][pl.ds(first, count), :] for k, first, count in sources], axis=0
        )
        picked = lax.dot_general(
            rows, pick_ref[...], (((0,), (0,)), ((), ())), preferred_element_type=jnp.float32
        )
        out_ref[:, pl.ds(block * paths, paths)] = (picked * factor).astype(jnp.bfloat16)


def right_own_kernel(layer_ref, projected_ref, out_ref):
    out_ref[...] = jnp.dot(
        layer_ref[...], projected_ref[...], preferred_element_type=jnp.float32
    ).astype(jnp.bfloat16)


def right_far_kernel(layer_ref, far_ref, here_ref, there_ref, mine_ref, near_ref, cross_ref):
    share, _ = mine_ref.shape
    half = near_ref.shape[0] - share
    start = pl.multiple_of(lax.axis_index("tile") * half, half)
    far = far_ref[...]
    mine_ref[...] = jnp.dot(
        far, here_ref[...], preferred_element_type=jnp.float32
    ).astype(jnp.bfloat16)
    cross = jnp.dot(far, there_ref[...], preferred_element_type=jnp.float32).astype(jnp.bfloat16)
    cross_ref[...] = cross
    near_ref[pl.ds(half, share), :] = cross
    near_ref[pl.ds(0, half), :] = jnp.dot(
        layer_ref[pl.ds(start, half), :], there_ref[...], preferred_element_type=jnp.float32
    ).astype(jnp.bfloat16)


def left_kernel(layer_ref, projected_ref, mine_ref, other_ref):
    paths = mine_ref.shape[1]
    states = jnp.dot(
        layer_ref[...], projected_ref[...], preferred_element_type=jnp.float32
    ).astype(jnp.bfloat16)
    mine_ref[...] = states[:, :paths]
    other_ref[...] = states[:, paths:]


def amplitude_kernel(left_pieces, left_count, *refs):
    left_refs, right_refs = refs[:left_count], refs[left_count:-4]
    out_ref, right_ref, block_ref, sems = refs[-4:]
    own_ref, mine_ref, x_ref, z_ref, xz_ref, mine_t_ref, x_t_ref, z_t_ref, xz_t_ref = right_refs
    path, tile, spot = lax.axis_index("path"), lax.axis_index("tile"), spot_of()
    tiles = lax.axis_size("tile")
    chunk, share = own_ref.shape[0], mine_ref.shape[0]
    half = z_ref.shape[0] - share

    def place(ref, first, count, plane, offset):
        start = pl.multiple_of((path ^ plane) * chunk + offset, count)
        right_ref[pl.ds(start, count), :] = ref[pl.ds(first, count), :]

    place(own_ref, 0, chunk, 0, 0)
    place(z_ref, 0, half, 1, tile * half)
    place(z_t_ref, 0, half, 1, (tile ^ 1) * half)
    for spin, (near_ref, x_piece, z_piece, xz_piece) in enumerate(
        ((mine_ref, x_ref, z_ref, xz_ref), (mine_t_ref, x_t_ref, z_t_ref, xz_t_ref))
    ):
        place(near_ref, 0, share, 2, (spot ^ spin) * share)
        place(x_piece, 0, share, 2, (spot ^ (spin + tiles)) * share)
        place(z_piece, half, share, 3, (spot ^ spin) * share)
        place(xz_piece, 0, share, 3, (spot ^ (spin + tiles)) * share)
    right = right_ref[...]
    copies = []
    for k, (source, first, count, spin, offset) in enumerate(left_pieces):
        block_ref[k, pl.ds(0, count), :] = lax.dot_general(
            left_refs[source][pl.ds(first, count), :],
            right,
            CONTRACT_LAST,
            preferred_element_type=jnp.float32,
        ).astype(jnp.bfloat16)
        start = pl.multiple_of((spot ^ spin) * chunk + offset, count)
        copy = pltpu.make_async_copy(
            block_ref.at[k, pl.ds(0, count), :], out_ref.at[pl.ds(start, count), :], sems.at[k]
        )
        copy.start()
        copies.append(copy)
    for copy in copies:
        copy.wait()


def exchanged(
    left_prefix, right_prefix, left_layer, right_layer, left_map, right_map, branch_bits, cut_side
):
    sizes = [lax.axis_size(axis) for axis in DEVICE_AXES]

    def exchange(value, plane=0, half=0, tile=0):
        pairs = []
        for p in range(sizes[0]):
            for h in range(sizes[1]):
                for t in range(sizes[2]):
                    source = (p * sizes[1] + h) * sizes[2] + t
                    target = ((p ^ plane) * sizes[1] + (h ^ half)) * sizes[2] + (t ^ tile)
                    pairs.append((source, target))
        return lax.ppermute(value, DEVICE_AXES, pairs)

    paths = left_map.shape[0]
    depth, gates = right_prefix.shape
    chunk = right_layer.shape[0]
    spots = sizes[1] * sizes[2]
    share = chunk // spots

    prefix_x = exchange(right_prefix, half=1)
    bits = branch_bits.T
    own, left_own, far_pack, codes = call(
        stage_kernel,
        [
            (depth, gates), (depth, gates), (share, gates),
            jax.ShapeDtypeStruct((8, paths), jnp.int32),
        ],
        right_prefix, left_prefix, right_layer,
        cut_side, bits, left_map[None, :], right_map[None, :],
        in_space=pltpu.HBM,
        scratch=(
            pltpu.SMEM(cut_side.shape, jnp.int32),
            pltpu.VMEM(bits.shape, jnp.int32),
            pltpu.VMEM((1, paths), jnp.int32),
            pltpu.VMEM((1, paths), jnp.int32),
            pltpu.SemaphoreType.DMA((7,)),
        ),
    )
    layer_x = exchange(left_layer, half=1)
    far = exchange(far_pack, plane=2)

    def join(sources, *arrays):
        count = sum(source[2] for source in sources)
        kernel = functools.partial(join_kernel, sources)
        return call(kernel, [(count, arrays[0].shape[1])], *arrays)[0]

    pair = join(((0, 0, depth), (1, 0, depth), (2, 0, depth)), own, prefix_x, left_own)
    near = exchange(pair, plane=1)
    pair_t = exchange(pair, tile=1)
    near_t = exchange(near, tile=1)
    left_factor, left_pick, right_factor, right_pick = call(
        mask_kernel,
        [(gates, paths), (sizes[0] * depth, paths), (gates, paths), (spots * depth, paths)],
        codes,
    )
    left_pair = join(((0, 2 * depth, depth), (1, 2 * depth, depth)), pair, near)
    left_far = exchange(left_pair, plane=2)
    left_far_t = exchange(left_far, tile=1)

    def project(sources, factor, pick, *arrays):
        kernel = functools.partial(project_kernel, sources)
        return call(kernel, [(gates, len(sources) * paths)], factor, pick, *arrays)[0]

    here = project(
        (((0, 0, depth), (1, 0, depth), (0, depth, depth), (1, depth, depth)),),
        right_factor, right_pick, pair, pair_t,
    )
    (right_near,) = call(right_own_kernel, [(chunk, paths)], right_layer, here)
    there = project(
        (((0, 0, depth), (1, 0, depth), (0, depth, depth), (1, depth, depth)),),
        right_factor, right_pick, near, near_t,
    )
    mine, for_near, cross = call(
        right_far_kernel,
        [(share, paths), (chunk // sizes[2] + share, paths), (share, paths)],
        right_layer, far, here, there,
    )
    right_pieces = [
        mine, exchange(mine, half=1), exchange(for_near, plane=1), exchange(cross, plane=1, half=1)
    ]
    right_pieces = right_pieces + [exchange(value, tile=1) for value in right_pieces]
    left_projected = project(
        (
            ((0, 0, 2 * depth), (1, 0, 2 * depth)),
            ((2, 2 * depth, depth), (3, 2 * depth, depth), (4, 0, 2 * depth)),
        ),
        left_factor, left_pick, left_pair, left_far, pair_t, near_t, left_far_t,
    )
    rows = left_layer.shape[0]
    own_mine, own_other = call(left_kernel, [(rows, paths)] * 2, left_layer, left_projected)
    x_mine, x_other = call(left_kernel, [(rows, paths)] * 2, layer_x, left_projected)
    left_states = [own_mine, exchange(own_other, tile=1), x_mine, exchange(x_other, tile=1)]
    left_pieces = tuple((k, 0, rows, spin, 0) for k, spin in enumerate((0, 1, 2, 3)))
    (amplitude,) = call(
        functools.partial(amplitude_kernel, left_pieces, len(left_states)),
        [(spots * rows, sizes[0] * chunk)],
        *left_states, right_near, *right_pieces,
        scratch=(
            pltpu.VMEM((sizes[0] * chunk, paths), jnp.bfloat16),
            pltpu.VMEM((len(left_pieces), rows, sizes[0] * chunk), jnp.bfloat16),
            pltpu.SemaphoreType.DMA((len(left_pieces),)),
        ),
        out_space=pl.ANY,
    )
    return amplitude


def solution(mesh):
    in_specs = (
        P(("groups", "path"), ("half", "tile")),
        P(("groups", "half", "tile"), "path"),
        P(("groups", "half", "tile"), None),
        P(("groups", "path"), None),
        P("groups"),
        P("groups"),
        P("groups", None),
        P("groups"),
    )
    out_specs = P(("groups", "half", "tile"), "path")
    squares = (mesh.shape["path"], mesh.shape["half"], mesh.shape["tile"]) == (4, 2, 2)

    def on_device(*arrays):
        return (exchanged if squares else gathered)(*arrays)

    return jax.shard_map(
        on_device, mesh=mesh, in_specs=in_specs, out_specs=out_specs, check_vma=False
    )
```

```python
import functools

import jax
import jax.numpy as jnp
from jax import lax
from jax.experimental import pallas as pl
from jax.experimental.pallas import tpu as pltpu
from jax.sharding import PartitionSpec as P


DEVICE_AXES = ("path", "half", "tile")
CONTRACT_LAST = (((1,), (1,)), ((), ()))


def cut_factors(branch, cut_side, gate_count, on_left):
    cut_count = cut_side.shape[0]
    bit_place = lax.broadcasted_iota(jnp.int32, (cut_count, gate_count), 0)
    gate_code = lax.broadcasted_iota(jnp.int32, (cut_count, gate_count), 1)
    bit_table = jnp.right_shift(gate_code, bit_place) & 1
    projector = cut_side if on_left else 1 - cut_side
    phased = 1 - projector
    chosen = branch * projector[None, :]
    misses = (
        jnp.sum(chosen, axis=1, keepdims=True)
        + jnp.dot(projector, bit_table)[None, :]
        - 2 * jnp.dot(chosen, bit_table)
    )
    parity = jnp.dot(branch * phased[None, :], bit_table)
    sign_value = 1 - 2 * (parity % 2)
    return jnp.where(misses == 0, sign_value, 0).astype(jnp.bfloat16)


def gathered(
    left_prefix, right_prefix, left_layer, right_layer, left_map, right_map, branch_bits, cut_side
):
    def states(prefix, prefix_axes, layer, layer_axes, path_map, on_left):
        rows = lax.all_gather(prefix, prefix_axes, axis=0, tiled=True)
        factor = cut_factors(branch_bits, cut_side, rows.shape[1], on_left)
        whole_layer = lax.all_gather(layer, layer_axes, axis=0, tiled=True)
        applied = lax.dot_general(
            rows[path_map] * factor, whole_layer, CONTRACT_LAST, preferred_element_type=jnp.float32
        )
        return applied.astype(jnp.bfloat16)

    left_states = states(left_prefix, "path", left_layer, ("half", "tile"), left_map, True)
    right_states = states(right_prefix, ("half", "tile"), right_layer, "path", right_map, False)
    amplitude = lax.dot_general(
        left_states, right_states, (((0,), (0,)), ((), ())), preferred_element_type=jnp.float32
    )
    return amplitude.astype(jnp.bfloat16)


def call(kernel, outs, *operands, in_space=pltpu.VMEM, scratch=(), out_space=pltpu.VMEM):
    shapes = [
        out_space(out, jnp.bfloat16) if isinstance(out, tuple) else out for out in outs
    ]
    spaces = [in_space] * len(operands)
    if in_space == pltpu.HBM:
        operands = [pltpu.with_memory_space_constraint(x, in_space) for x in operands]
    return pl.pallas_call(
        kernel,
        out_shape=shapes,
        in_specs=[pl.BlockSpec(memory_space=space) for space in spaces],
        out_specs=[pl.BlockSpec(memory_space=out_space)] * len(shapes),
        scratch_shapes=list(scratch),
        compiler_params=pltpu.CompilerParams(vmem_limit_bytes=16 << 20),
    )(*operands)


def spot_of():
    return lax.axis_index("half") * lax.axis_size("tile") + lax.axis_index("tile")


def stage_kernel(*refs):
    layer_ref, sources, targets, sems = refs[0], refs[1:7], refs[8:14], refs[14]
    far_ref = refs[7]
    share = far_ref.shape[0]
    order = lax.axis_index("tile") * lax.axis_size("half") + lax.axis_index("half")
    start = pl.multiple_of(order * share, share)
    copies = [pltpu.make_async_copy(layer_ref.at[pl.ds(start, share), :], far_ref, sems.at[0])]
    for k, (source, target) in enumerate(zip(sources, targets)):
        copies.append(pltpu.make_async_copy(source, target, sems.at[k + 1]))
    for copy in copies:
        copy.start()
    for copy in copies:
        copy.wait()


def mask_kernel(side_ref, branch_ref, left_map_ref, right_map_ref, *out_refs):
    cuts, paths = branch_ref.shape
    for half, (map_ref, shard, shards) in enumerate(
        (
            (left_map_ref, lax.axis_index("path"), lax.axis_size("path")),
            (right_map_ref, spot_of(), lax.axis_size("half") * lax.axis_size("tile")),
        )
    ):
        factor_ref, pick_ref = out_refs[2 * half:][:2]
        wanted = jnp.zeros((1, paths), jnp.int32)
        phased = jnp.zeros((1, paths), jnp.int32)
        mask = jnp.zeros((1, 1), jnp.int32)
        for cut in range(cuts):
            side = side_ref[:, pl.ds(cut, 1)]
            projector = 1 - side if half else side
            bits = branch_ref[pl.ds(cut, 1), :]
            wanted += bits * (projector << cut)
            phased += bits * ((1 - projector) << cut)
            mask += projector << cut
        depth = pick_ref.shape[0] // shards
        row = map_ref[...]
        place = (lax.div(row, depth) ^ shard) * depth + lax.rem(row, depth)
        gate = lax.broadcasted_iota(jnp.int32, factor_ref.shape, 0)
        hit = (gate & mask) == wanted
        odd = (lax.population_count(gate & phased) & 1) == 1
        factor = jnp.where(hit, jnp.where(odd, -1.0, 1.0), 0.0)
        factor_ref[...] = factor.astype(jnp.bfloat16)
        index = lax.broadcasted_iota(jnp.int32, pick_ref.shape, 0)
        pick_ref[...] = jnp.where(index == place, 1.0, 0.0).astype(jnp.bfloat16)


def join_kernel(sources, *refs):
    out_ref, at = refs[-1], 0
    for k, first, count in sources:
        out_ref[pl.ds(at, count), :] = refs[k][pl.ds(first, count), :]
        at += count


def project_kernel(pieces, factor_ref, pick_ref, *refs):
    prefix_refs, out_ref = refs[:-1], refs[-1]
    paths = pick_ref.shape[1]
    factor = factor_ref[...].astype(jnp.float32)
    for block, sources in enumerate(pieces):
        rows = jnp.concatenate(
            [prefix_refs[k][pl.ds(first, count), :] for k, first, count in sources], axis=0
        )
        picked = lax.dot_general(
            rows, pick_ref[...], (((0,), (0,)), ((), ())), preferred_element_type=jnp.float32
        )
        out_ref[:, pl.ds(block * paths, paths)] = (picked * factor).astype(jnp.bfloat16)


def right_own_kernel(layer_ref, projected_ref, out_ref):
    out_ref[...] = jnp.dot(
        layer_ref[...], projected_ref[...], preferred_element_type=jnp.float32
    ).astype(jnp.bfloat16)


def right_far_kernel(layer_ref, far_ref, here_ref, there_ref, mine_ref, near_ref, cross_ref):
    share, _ = mine_ref.shape
    half = near_ref.shape[0] - share
    start = pl.multiple_of(lax.axis_index("tile") * half, half)
    far = far_ref[...]
    mine_ref[...] = jnp.dot(
        far, here_ref[...], preferred_element_type=jnp.float32
    ).astype(jnp.bfloat16)
    cross = jnp.dot(far, there_ref[...], preferred_element_type=jnp.float32).astype(jnp.bfloat16)
    cross_ref[...] = cross
    near_ref[pl.ds(half, share), :] = cross
    near_ref[pl.ds(0, half), :] = jnp.dot(
        layer_ref[pl.ds(start, half), :], there_ref[...], preferred_element_type=jnp.float32
    ).astype(jnp.bfloat16)


def left_kernel(own_ref, x_ref, projected_ref, mine_ref, other_ref):
    rows, paths = own_ref.shape[0], mine_ref.shape[1]
    for k, layer_ref in enumerate((own_ref, x_ref)):
        states = jnp.dot(
            layer_ref[...], projected_ref[...], preferred_element_type=jnp.float32
        ).astype(jnp.bfloat16)
        mine_ref[pl.ds(k * rows, rows), :] = states[:, :paths]
        other_ref[pl.ds(k * rows, rows), :] = states[:, paths:]


def join_right(right_ref, at, mine_ref, x_ref, z_ref, xz_ref):
    half, share = lax.axis_index("half"), mine_ref.shape[0]
    side = z_ref.shape[0] - share
    right_ref[pl.ds(at, side), :] = z_ref[pl.ds(0, side), :]
    for plane, near_ref, first, far_ref in ((2, mine_ref, 0, x_ref), (3, z_ref, side, xz_ref)):
        base = at + (plane - 1) * side
        right_ref[pl.ds(pl.multiple_of(base + half * share, share), share), :] = near_ref[
            pl.ds(first, share), :
        ]
        right_ref[pl.ds(pl.multiple_of(base + (half ^ 1) * share, share), share), :] = far_ref[...]


def left_blocks(left_refs):
    for tile, ref in enumerate(left_refs):
        rows = ref.shape[0] // 2
        for half in range(2):
            spin = half * lax.axis_size("tile") + tile
            row = pl.multiple_of((spot_of() ^ spin) * rows, rows)
            yield ref[pl.ds(half * rows, rows), :], rows, row


def amplitude_near_kernel(left_count, *refs):
    left_refs, right_refs, (out_ref, right_ref) = refs[:left_count], refs[left_count:-2], refs[-2:]
    chunk = right_refs[0].shape[0]
    right_ref[pl.ds(0, chunk), :] = right_refs[0][...]
    join_right(right_ref, chunk, *right_refs[1:])
    right = right_ref[...]
    for left, rows, row in left_blocks(left_refs):
        out_ref[pl.ds(row, rows), :] = lax.dot_general(
            left, right, CONTRACT_LAST, preferred_element_type=jnp.float32
        ).astype(jnp.bfloat16)


def amplitude_rest_kernel(left_count, near_ref, *refs):
    left_refs, right_refs = refs[:left_count], refs[left_count:-4]
    out_ref, right_ref, block_ref, sems = refs[-4:]
    path, tile = lax.axis_index("path"), lax.axis_index("tile")
    side = right_ref.shape[0] // 3
    chunk = side * lax.axis_size("tile")
    copies = []

    def send(source, row, rows, column, width):
        place = pl.ds(row, rows), pl.ds(pl.multiple_of(column, side), width)
        copy = pltpu.make_async_copy(source, out_ref.at[place], sems.at[len(copies)])
        copies.append(copy)
        copy.start()

    height = near_ref.shape[0]
    send(near_ref.at[:, pl.ds(0, chunk)], 0, height, path * chunk, chunk)
    for plane in range(1, 4):
        source = near_ref.at[:, pl.ds(chunk + (plane - 1) * side, side)]
        send(source, 0, height, (path ^ plane) * chunk + tile * side, side)
    join_right(right_ref, 0, *right_refs)
    right = right_ref[...]
    for k, (left, rows, row) in enumerate(left_blocks(left_refs)):
        block_ref[k] = lax.dot_general(
            left, right, CONTRACT_LAST, preferred_element_type=jnp.float32
        ).astype(jnp.bfloat16)
        for plane in range(1, 4):
            source = block_ref.at[k, :, pl.ds((plane - 1) * side, side)]
            send(source, row, rows, (path ^ plane) * chunk + (tile ^ 1) * side, side)
    for copy in copies:
        copy.wait()


def exchanged(
    left_prefix, right_prefix, left_layer, right_layer, left_map, right_map, branch_bits, cut_side
):
    sizes = [lax.axis_size(axis) for axis in DEVICE_AXES]

    def exchange(value, plane=0, half=0, tile=0):
        pairs = []
        for p in range(sizes[0]):
            for h in range(sizes[1]):
                for t in range(sizes[2]):
                    source = (p * sizes[1] + h) * sizes[2] + t
                    target = ((p ^ plane) * sizes[1] + (h ^ half)) * sizes[2] + (t ^ tile)
                    pairs.append((source, target))
        return lax.ppermute(value, DEVICE_AXES, pairs)

    paths = left_map.shape[0]
    depth, gates = right_prefix.shape
    chunk = right_layer.shape[0]
    spots = sizes[1] * sizes[2]
    share = chunk // spots

    prefix_x = exchange(right_prefix, half=1)
    small = (cut_side[None, :], branch_bits.T, left_map[None, :], right_map[None, :])
    far_pack, own, left_own, *small = call(
        stage_kernel,
        [(share, gates), (depth, gates), (depth, gates)]
        + [jax.ShapeDtypeStruct(x.shape, x.dtype) for x in small],
        right_layer, right_prefix, left_prefix, *small,
        in_space=pltpu.HBM,
        scratch=(pltpu.SemaphoreType.DMA((7,)),),
    )
    layer_x = exchange(left_layer, half=1)
    far = exchange(far_pack, plane=2)

    def join(sources, *arrays):
        count = sum(source[2] for source in sources)
        kernel = functools.partial(join_kernel, sources)
        return call(kernel, [(count, arrays[0].shape[1])], *arrays)[0]

    pair = join(((0, 0, depth), (1, 0, depth), (2, 0, depth)), own, prefix_x, left_own)
    near = exchange(pair, plane=1)
    pair_t = exchange(pair, tile=1)
    near_t = exchange(near, tile=1)
    left_factor, left_pick, right_factor, right_pick = call(
        mask_kernel,
        [(gates, paths), (sizes[0] * depth, paths), (gates, paths), (spots * depth, paths)],
        *small,
    )
    left_pair = join(((0, 2 * depth, depth), (1, 2 * depth, depth)), pair, near)
    left_far = exchange(left_pair, plane=2)
    left_far_t = exchange(left_far, tile=1)

    def project(sources, factor, pick, *arrays):
        kernel = functools.partial(project_kernel, sources)
        return call(kernel, [(gates, len(sources) * paths)], factor, pick, *arrays)[0]

    here = project(
        (((0, 0, depth), (1, 0, depth), (0, depth, depth), (1, depth, depth)),),
        right_factor, right_pick, pair, pair_t,
    )
    (right_near,) = call(right_own_kernel, [(chunk, paths)], right_layer, here)
    there = project(
        (((0, 0, depth), (1, 0, depth), (0, depth, depth), (1, depth, depth)),),
        right_factor, right_pick, near, near_t,
    )
    mine, for_near, cross = call(
        right_far_kernel,
        [(share, paths), (chunk // sizes[2] + share, paths), (share, paths)],
        right_layer, far, here, there,
    )
    right_pieces = [
        mine, exchange(mine, half=1), exchange(for_near, plane=1), exchange(cross, plane=1, half=1)
    ]
    right_pieces_t = [exchange(piece, tile=1) for piece in right_pieces]
    left_projected = project(
        (
            ((0, 0, 2 * depth), (1, 0, 2 * depth)),
            ((2, 2 * depth, depth), (3, 2 * depth, depth), (4, 0, 2 * depth)),
        ),
        left_factor, left_pick, left_pair, left_far, pair_t, near_t, left_far_t,
    )
    rows = left_layer.shape[0]
    left_mine, left_other = call(
        left_kernel, [(2 * rows, paths)] * 2, left_layer, layer_x, left_projected
    )
    left_states = [left_mine, exchange(left_other, tile=1)]
    side = chunk // sizes[2]
    height = spots * rows
    (amplitude,) = call(
        functools.partial(amplitude_near_kernel, len(left_states)),
        [(height, chunk + 3 * side)],
        *left_states, right_near, *right_pieces,
        scratch=(pltpu.VMEM((chunk + 3 * side, paths), jnp.bfloat16),),
    )
    return call(
        functools.partial(amplitude_rest_kernel, len(left_states)),
        [(height, sizes[0] * chunk)],
        amplitude, *left_states, *right_pieces_t,
        scratch=(
            pltpu.VMEM((3 * side, paths), jnp.bfloat16),
            pltpu.VMEM((spots, rows, 3 * side), jnp.bfloat16),
            pltpu.SemaphoreType.DMA((4 + 3 * spots,)),
        ),
        out_space=pltpu.HBM,
    )[0]


def solution(mesh):
    in_specs = (
        P(("groups", "path"), ("half", "tile")),
        P(("groups", "half", "tile"), "path"),
        P(("groups", "half", "tile"), None),
        P(("groups", "path"), None),
        P("groups"),
        P("groups"),
        P("groups", None),
        P("groups"),
    )
    out_specs = P(("groups", "half", "tile"), "path")
    squares = (mesh.shape["path"], mesh.shape["half"], mesh.shape["tile"]) == (4, 2, 2)

    def on_device(*arrays):
        return (exchanged if squares else gathered)(*arrays)

    return jax.shard_map(
        on_device, mesh=mesh, in_specs=in_specs, out_specs=out_specs, check_vma=False
    )
```

```python
import functools

import jax
import jax.numpy as jnp
from jax import lax
from jax.experimental import pallas as pl
from jax.experimental.pallas import tpu as pltpu
from jax.sharding import PartitionSpec as P


DEVICE_AXES = ("path", "half", "tile")
CONTRACT_LAST = (((1,), (1,)), ((), ()))


def cut_factors(branch, cut_side, gate_count, on_left):
    cut_count = cut_side.shape[0]
    bit_place = lax.broadcasted_iota(jnp.int32, (cut_count, gate_count), 0)
    gate_code = lax.broadcasted_iota(jnp.int32, (cut_count, gate_count), 1)
    bit_table = jnp.right_shift(gate_code, bit_place) & 1
    projector = cut_side if on_left else 1 - cut_side
    phased = 1 - projector
    chosen = branch * projector[None, :]
    misses = (
        jnp.sum(chosen, axis=1, keepdims=True)
        + jnp.dot(projector, bit_table)[None, :]
        - 2 * jnp.dot(chosen, bit_table)
    )
    parity = jnp.dot(branch * phased[None, :], bit_table)
    sign_value = 1 - 2 * (parity % 2)
    return jnp.where(misses == 0, sign_value, 0).astype(jnp.bfloat16)


def gathered(
    left_prefix, right_prefix, left_layer, right_layer, left_map, right_map, branch_bits, cut_side
):
    def states(prefix, prefix_axes, layer, layer_axes, path_map, on_left):
        rows = lax.all_gather(prefix, prefix_axes, axis=0, tiled=True)
        factor = cut_factors(branch_bits, cut_side, rows.shape[1], on_left)
        whole_layer = lax.all_gather(layer, layer_axes, axis=0, tiled=True)
        applied = lax.dot_general(
            rows[path_map] * factor, whole_layer, CONTRACT_LAST, preferred_element_type=jnp.float32
        )
        return applied.astype(jnp.bfloat16)

    left_states = states(left_prefix, "path", left_layer, ("half", "tile"), left_map, True)
    right_states = states(right_prefix, ("half", "tile"), right_layer, "path", right_map, False)
    amplitude = lax.dot_general(
        left_states, right_states, (((0,), (0,)), ((), ())), preferred_element_type=jnp.float32
    )
    return amplitude.astype(jnp.bfloat16)


def call(kernel, outs, *operands, in_space=pltpu.VMEM, scratch=(), out_space=pltpu.VMEM):
    shapes = [
        out_space(out, jnp.bfloat16) if isinstance(out, tuple) else out for out in outs
    ]
    spaces = [in_space] * len(operands)
    if in_space == pltpu.HBM:
        operands = [pltpu.with_memory_space_constraint(x, in_space) for x in operands]
    return pl.pallas_call(
        kernel,
        out_shape=shapes,
        in_specs=[pl.BlockSpec(memory_space=space) for space in spaces],
        out_specs=[pl.BlockSpec(memory_space=out_space)] * len(shapes),
        scratch_shapes=list(scratch),
        compiler_params=pltpu.CompilerParams(vmem_limit_bytes=16 << 20),
    )(*operands)


def spot_of():
    return lax.axis_index("half") * lax.axis_size("tile") + lax.axis_index("tile")


def stage_kernel(*refs):
    layer_ref, sources, targets, sems = refs[0], refs[1:7], refs[8:14], refs[14]
    far_ref = refs[7]
    share = far_ref.shape[0]
    order = lax.axis_index("tile") * lax.axis_size("half") + lax.axis_index("half")
    start = pl.multiple_of(order * share, share)
    copies = [pltpu.make_async_copy(layer_ref.at[pl.ds(start, share), :], far_ref, sems.at[0])]
    for k, (source, target) in enumerate(zip(sources, targets)):
        copies.append(pltpu.make_async_copy(source, target, sems.at[k + 1]))
    for copy in copies:
        copy.start()
    for copy in copies:
        copy.wait()


def mask_kernel(side_ref, branch_ref, left_map_ref, right_map_ref, *out_refs):
    cuts, paths = branch_ref.shape
    for half, (map_ref, shard, shards) in enumerate(
        (
            (left_map_ref, lax.axis_index("path"), lax.axis_size("path")),
            (right_map_ref, spot_of(), lax.axis_size("half") * lax.axis_size("tile")),
        )
    ):
        factor_ref, pick_ref = out_refs[2 * half:][:2]
        wanted = jnp.zeros((1, paths), jnp.int32)
        phased = jnp.zeros((1, paths), jnp.int32)
        mask = jnp.zeros((1, 1), jnp.int32)
        for cut in range(cuts):
            side = side_ref[:, pl.ds(cut, 1)]
            projector = 1 - side if half else side
            bits = branch_ref[pl.ds(cut, 1), :]
            wanted += bits * (projector << cut)
            phased += bits * ((1 - projector) << cut)
            mask += projector << cut
        depth = pick_ref.shape[0] // shards
        row = map_ref[...]
        place = (lax.div(row, depth) ^ shard) * depth + lax.rem(row, depth)
        gate = lax.broadcasted_iota(jnp.int32, factor_ref.shape, 0)
        hit = (gate & mask) == wanted
        odd = (lax.population_count(gate & phased) & 1) == 1
        factor = jnp.where(hit, jnp.where(odd, -1.0, 1.0), 0.0)
        factor_ref[...] = factor.astype(jnp.bfloat16)
        index = lax.broadcasted_iota(jnp.int32, pick_ref.shape, 0)
        pick_ref[...] = jnp.where(index == place, 1.0, 0.0).astype(jnp.bfloat16)


def join_kernel(sources, *refs):
    out_ref, at = refs[-1], 0
    for k, first, count in sources:
        out_ref[pl.ds(at, count), :] = refs[k][pl.ds(first, count), :]
        at += count


def project_kernel(pieces, factor_ref, pick_ref, *refs):
    prefix_refs, out_ref = refs[:-1], refs[-1]
    paths = pick_ref.shape[1]
    factor = factor_ref[...].astype(jnp.float32)
    for block, sources in enumerate(pieces):
        rows = jnp.concatenate(
            [prefix_refs[k][pl.ds(first, count), :] for k, first, count in sources], axis=0
        )
        picked = lax.dot_general(
            rows, pick_ref[...], (((0,), (0,)), ((), ())), preferred_element_type=jnp.float32
        )
        out_ref[:, pl.ds(block * paths, paths)] = (picked * factor).astype(jnp.bfloat16)


def right_own_kernel(layer_ref, projected_ref, out_ref):
    out_ref[...] = jnp.dot(
        layer_ref[...], projected_ref[...], preferred_element_type=jnp.float32
    ).astype(jnp.bfloat16)


def right_far_kernel(layer_ref, far_ref, here_ref, there_ref, both_ref, near_ref):
    share = far_ref.shape[0]
    half = near_ref.shape[0] - share
    start = pl.multiple_of(lax.axis_index("tile") * half, half)
    far = far_ref[...]
    both_ref[pl.ds(0, share), :] = jnp.dot(
        far, here_ref[...], preferred_element_type=jnp.float32
    ).astype(jnp.bfloat16)
    cross = jnp.dot(far, there_ref[...], preferred_element_type=jnp.float32).astype(jnp.bfloat16)
    both_ref[pl.ds(share, share), :] = cross
    near_ref[pl.ds(half, share), :] = cross
    near_ref[pl.ds(0, half), :] = jnp.dot(
        layer_ref[pl.ds(start, half), :], there_ref[...], preferred_element_type=jnp.float32
    ).astype(jnp.bfloat16)


def mix_kernel(both_ref, both_t_ref, out_ref):
    share = out_ref.shape[0] // 2
    first = pl.multiple_of(lax.axis_index("tile") * share, share)
    out_ref[pl.ds(0, share), :] = both_ref[pl.ds(first, share), :]
    out_ref[pl.ds(share, share), :] = both_t_ref[pl.ds(first, share), :]


def left_kernel(own_ref, x_ref, projected_ref, mine_ref, other_ref):
    rows, paths = own_ref.shape[0], mine_ref.shape[1]
    for k, layer_ref in enumerate((own_ref, x_ref)):
        states = jnp.dot(
            layer_ref[...], projected_ref[...], preferred_element_type=jnp.float32
        ).astype(jnp.bfloat16)
        mine_ref[pl.ds(k * rows, rows), :] = states[:, :paths]
        other_ref[pl.ds(k * rows, rows), :] = states[:, paths:]


def left_blocks(left_refs):
    for tile, ref in enumerate(left_refs):
        rows = ref.shape[0] // 2
        for half in range(2):
            spin = half * lax.axis_size("tile") + tile
            row = pl.multiple_of((spot_of() ^ spin) * rows, rows)
            yield ref[pl.ds(half * rows, rows), :], rows, row


def amplitude_near_kernel(left_count, *refs):
    left_refs, (own_ref, z_ref, out_ref, right_ref) = refs[:left_count], refs[left_count:]
    chunk = own_ref.shape[0]
    side = right_ref.shape[0] - chunk
    right_ref[pl.ds(0, chunk), :] = own_ref[...]
    right_ref[pl.ds(chunk, side), :] = z_ref[pl.ds(0, side), :]
    right = right_ref[...]
    for left, rows, row in left_blocks(left_refs):
        out_ref[pl.ds(row, rows), :] = lax.dot_general(
            left, right, CONTRACT_LAST, preferred_element_type=jnp.float32
        ).astype(jnp.bfloat16)


def amplitude_rest_kernel(left_count, near_ref, *refs):
    left_refs, right_refs = refs[:left_count], refs[left_count:-4]
    out_ref, right_ref, block_ref, sems = refs[-4:]
    both_ref, mixed_ref, z_ref, both_t_ref, mixed_t_ref, z_t_ref = right_refs
    path, half, tile = (lax.axis_index(axis) for axis in DEVICE_AXES)
    share, halves = both_ref.shape[0] // 2, lax.axis_size("half")
    side = z_ref.shape[0] - share
    chunk = side * lax.axis_size("tile")

    def place(ref, first, far, core, column_half):
        start = side + far * chunk + (core * halves + column_half) * share
        right_ref[pl.ds(pl.multiple_of(start, share), share), :] = ref[pl.ds(first, share), :]

    right_ref[pl.ds(0, side), :] = z_t_ref[pl.ds(0, side), :]
    for core, near, mixed, z in (
        (tile, both_ref, mixed_ref, z_ref), (tile ^ 1, both_t_ref, mixed_t_ref, z_t_ref)
    ):
        place(near, 0, 0, core, half)
        place(z, side, 1, core, half)
        place(mixed, 0, core, core, half ^ 1)
        place(mixed, share, core, core ^ 1, half ^ 1)
    copies = []

    def send(source, row, rows, column, width):
        place = pl.ds(row, rows), pl.ds(pl.multiple_of(column, side), width)
        copy = pltpu.make_async_copy(source, out_ref.at[place], sems.at[len(copies)])
        copies.append(copy)
        copy.start()

    height = near_ref.shape[0]
    send(near_ref.at[:, pl.ds(0, chunk)], 0, height, path * chunk, chunk)
    source = near_ref.at[:, pl.ds(chunk, side)]
    send(source, 0, height, (path ^ 1) * chunk + tile * side, side)
    right = right_ref[...]
    for k, (left, rows, row) in enumerate(left_blocks(left_refs)):
        block_ref[k] = lax.dot_general(
            left, right, CONTRACT_LAST, preferred_element_type=jnp.float32
        ).astype(jnp.bfloat16)
        column = (path ^ 1) * chunk + (tile ^ 1) * side
        send(block_ref.at[k, :, pl.ds(0, side)], row, rows, column, side)
        for far in range(2):
            source = block_ref.at[k, :, pl.ds(side + far * chunk, chunk)]
            send(source, row, rows, (path ^ (2 + far)) * chunk, chunk)
    for copy in copies:
        copy.wait()


def exchanged(
    left_prefix, right_prefix, left_layer, right_layer, left_map, right_map, branch_bits, cut_side
):
    sizes = [lax.axis_size(axis) for axis in DEVICE_AXES]

    def exchange(value, plane=0, half=0, tile=0, tile_plane=0):
        pairs = []
        for p in range(sizes[0]):
            for h in range(sizes[1]):
                for t in range(sizes[2]):
                    source = (p * sizes[1] + h) * sizes[2] + t
                    q = p ^ plane ^ (tile_plane * t)
                    target = (q * sizes[1] + (h ^ half)) * sizes[2] + (t ^ tile)
                    pairs.append((source, target))
        return lax.ppermute(value, DEVICE_AXES, pairs)

    paths = left_map.shape[0]
    depth, gates = right_prefix.shape
    chunk = right_layer.shape[0]
    spots = sizes[1] * sizes[2]
    share = chunk // spots

    prefix_x = exchange(right_prefix, half=1)
    small = (cut_side[None, :], branch_bits.T, left_map[None, :], right_map[None, :])
    far_pack, own, left_own, *small = call(
        stage_kernel,
        [(share, gates), (depth, gates), (depth, gates)]
        + [jax.ShapeDtypeStruct(x.shape, x.dtype) for x in small],
        right_layer, right_prefix, left_prefix, *small,
        in_space=pltpu.HBM,
        scratch=(pltpu.SemaphoreType.DMA((7,)),),
    )
    layer_x = exchange(left_layer, half=1)
    far = exchange(far_pack, plane=2)

    def join(sources, *arrays):
        count = sum(source[2] for source in sources)
        kernel = functools.partial(join_kernel, sources)
        return call(kernel, [(count, arrays[0].shape[1])], *arrays)[0]

    pair = join(((0, 0, depth), (1, 0, depth), (2, 0, depth)), own, prefix_x, left_own)
    near = exchange(pair, plane=1)
    pair_t = exchange(pair, tile=1)
    near_t = exchange(near, tile=1)
    left_factor, left_pick, right_factor, right_pick = call(
        mask_kernel,
        [(gates, paths), (sizes[0] * depth, paths), (gates, paths), (spots * depth, paths)],
        *small,
    )
    left_pair = join(((0, 2 * depth, depth), (1, 2 * depth, depth)), pair, near)
    left_far = exchange(left_pair, plane=2)
    left_far_t = exchange(left_far, tile=1)

    def project(sources, factor, pick, *arrays):
        kernel = functools.partial(project_kernel, sources)
        return call(kernel, [(gates, len(sources) * paths)], factor, pick, *arrays)[0]

    here = project(
        (((0, 0, depth), (1, 0, depth), (0, depth, depth), (1, depth, depth)),),
        right_factor, right_pick, pair, pair_t,
    )
    (right_near,) = call(right_own_kernel, [(chunk, paths)], right_layer, here)
    there = project(
        (((0, 0, depth), (1, 0, depth), (0, depth, depth), (1, depth, depth)),),
        right_factor, right_pick, near, near_t,
    )
    both, for_near = call(
        right_far_kernel,
        [(2 * share, paths), (chunk // sizes[2] + share, paths)],
        right_layer, far, here, there,
    )
    both_t = exchange(both, tile=1)
    from_z = exchange(for_near, plane=1)
    (mix,) = call(mix_kernel, [(2 * share, paths)], both, both_t)
    mixed = exchange(mix, half=1, tile_plane=1)
    right_pieces = [
        both, mixed, from_z,
        both_t, exchange(mixed, tile=1), exchange(from_z, tile=1),
    ]
    left_projected = project(
        (
            ((0, 0, 2 * depth), (1, 0, 2 * depth)),
            ((2, 2 * depth, depth), (3, 2 * depth, depth), (4, 0, 2 * depth)),
        ),
        left_factor, left_pick, left_pair, left_far, pair_t, near_t, left_far_t,
    )
    rows = left_layer.shape[0]
    left_mine, left_other = call(
        left_kernel, [(2 * rows, paths)] * 2, left_layer, layer_x, left_projected
    )
    left_states = [left_mine, exchange(left_other, tile=1)]
    side = chunk // sizes[2]
    height = spots * rows
    (amplitude,) = call(
        functools.partial(amplitude_near_kernel, len(left_states)),
        [(height, chunk + side)],
        *left_states, right_near, from_z,
        scratch=(pltpu.VMEM((chunk + side, paths), jnp.bfloat16),),
    )
    return call(
        functools.partial(amplitude_rest_kernel, len(left_states)),
        [(height, sizes[0] * chunk)],
        amplitude, *left_states, *right_pieces,
        scratch=(
            pltpu.VMEM((2 * chunk + side, paths), jnp.bfloat16),
            pltpu.VMEM((spots, rows, 2 * chunk + side), jnp.bfloat16),
            pltpu.SemaphoreType.DMA((2 + 3 * spots,)),
        ),
        out_space=pltpu.HBM,
    )[0]


def solution(mesh):
    in_specs = (
        P(("groups", "path"), ("half", "tile")),
        P(("groups", "half", "tile"), "path"),
        P(("groups", "half", "tile"), None),
        P(("groups", "path"), None),
        P("groups"),
        P("groups"),
        P("groups", None),
        P("groups"),
    )
    out_specs = P(("groups", "half", "tile"), "path")
    squares = (mesh.shape["path"], mesh.shape["half"], mesh.shape["tile"]) == (4, 2, 2)

    def on_device(*arrays):
        return (exchanged if squares else gathered)(*arrays)

    return jax.shard_map(
        on_device, mesh=mesh, in_specs=in_specs, out_specs=out_specs, check_vma=False
    )
```

```python
import functools

import jax
import jax.numpy as jnp
from jax import lax
from jax.experimental import pallas as pl
from jax.experimental.pallas import tpu as pltpu
from jax.sharding import PartitionSpec as P


DEVICE_AXES = ("path", "half", "tile")
CONTRACT_LAST = (((1,), (1,)), ((), ()))


def cut_factors(branch, cut_side, gate_count, on_left):
    cut_count = cut_side.shape[0]
    bit_place = lax.broadcasted_iota(jnp.int32, (cut_count, gate_count), 0)
    gate_code = lax.broadcasted_iota(jnp.int32, (cut_count, gate_count), 1)
    bit_table = jnp.right_shift(gate_code, bit_place) & 1
    projector = cut_side if on_left else 1 - cut_side
    phased = 1 - projector
    chosen = branch * projector[None, :]
    misses = (
        jnp.sum(chosen, axis=1, keepdims=True)
        + jnp.dot(projector, bit_table)[None, :]
        - 2 * jnp.dot(chosen, bit_table)
    )
    parity = jnp.dot(branch * phased[None, :], bit_table)
    sign_value = 1 - 2 * (parity % 2)
    return jnp.where(misses == 0, sign_value, 0).astype(jnp.bfloat16)


def gathered(
    left_prefix, right_prefix, left_layer, right_layer, left_map, right_map, branch_bits, cut_side
):
    def states(prefix, prefix_axes, layer, layer_axes, path_map, on_left):
        rows = lax.all_gather(prefix, prefix_axes, axis=0, tiled=True)
        factor = cut_factors(branch_bits, cut_side, rows.shape[1], on_left)
        whole_layer = lax.all_gather(layer, layer_axes, axis=0, tiled=True)
        applied = lax.dot_general(
            rows[path_map] * factor, whole_layer, CONTRACT_LAST, preferred_element_type=jnp.float32
        )
        return applied.astype(jnp.bfloat16)

    left_states = states(left_prefix, "path", left_layer, ("half", "tile"), left_map, True)
    right_states = states(right_prefix, ("half", "tile"), right_layer, "path", right_map, False)
    amplitude = lax.dot_general(
        left_states, right_states, (((0,), (0,)), ((), ())), preferred_element_type=jnp.float32
    )
    return amplitude.astype(jnp.bfloat16)


def call(kernel, outs, *operands, in_space=pltpu.VMEM, scratch=(), out_space=pltpu.VMEM):
    shapes = [
        out_space(out, jnp.bfloat16) if isinstance(out, tuple) else out for out in outs
    ]
    spaces = [in_space] * len(operands)
    if in_space == pltpu.HBM:
        operands = [pltpu.with_memory_space_constraint(x, in_space) for x in operands]
    return pl.pallas_call(
        kernel,
        out_shape=shapes,
        in_specs=[pl.BlockSpec(memory_space=space) for space in spaces],
        out_specs=[pl.BlockSpec(memory_space=out_space)] * len(shapes),
        scratch_shapes=list(scratch),
        compiler_params=pltpu.CompilerParams(vmem_limit_bytes=16 << 20),
    )(*operands)


def spot_of():
    return lax.axis_index("half") * lax.axis_size("tile") + lax.axis_index("tile")


def stage_kernel(*refs):
    layer_ref, sources, targets, sems = refs[0], refs[1:7], refs[8:14], refs[14]
    far_ref = refs[7]
    share = far_ref.shape[0]
    order = lax.axis_index("tile") * lax.axis_size("half") + lax.axis_index("half")
    start = pl.multiple_of(order * share, share)
    copies = [pltpu.make_async_copy(layer_ref.at[pl.ds(start, share), :], far_ref, sems.at[0])]
    for k, (source, target) in enumerate(zip(sources, targets)):
        copies.append(pltpu.make_async_copy(source, target, sems.at[k + 1]))
    for copy in copies:
        copy.start()
    for copy in copies:
        copy.wait()


def mask_kernel(side_ref, branch_ref, left_map_ref, right_map_ref, *out_refs):
    cuts, paths = branch_ref.shape
    for half, (map_ref, shard, shards) in enumerate(
        (
            (left_map_ref, lax.axis_index("path"), lax.axis_size("path")),
            (right_map_ref, spot_of(), lax.axis_size("half") * lax.axis_size("tile")),
        )
    ):
        factor_ref, pick_ref = out_refs[2 * half:][:2]
        wanted = jnp.zeros((1, paths), jnp.int32)
        phased = jnp.zeros((1, paths), jnp.int32)
        mask = jnp.zeros((1, 1), jnp.int32)
        for cut in range(cuts):
            side = side_ref[:, pl.ds(cut, 1)]
            projector = 1 - side if half else side
            bits = branch_ref[pl.ds(cut, 1), :]
            wanted += bits * (projector << cut)
            phased += bits * ((1 - projector) << cut)
            mask += projector << cut
        depth = pick_ref.shape[0] // shards
        row = map_ref[...]
        place = (lax.div(row, depth) ^ shard) * depth + lax.rem(row, depth)
        gate = lax.broadcasted_iota(jnp.int32, factor_ref.shape, 0)
        hit = (gate & mask) == wanted
        odd = (lax.population_count(gate & phased) & 1) == 1
        factor = jnp.where(hit, jnp.where(odd, -1.0, 1.0), 0.0)
        factor_ref[...] = factor.astype(jnp.bfloat16)
        index = lax.broadcasted_iota(jnp.int32, pick_ref.shape, 0)
        pick_ref[...] = jnp.where(index == place, 1.0, 0.0).astype(jnp.bfloat16)


def join_kernel(sources, *refs):
    out_ref, at = refs[-1], 0
    for k, first, count in sources:
        out_ref[pl.ds(at, count), :] = refs[k][pl.ds(first, count), :]
        at += count


def project_kernel(pieces, factor_ref, pick_ref, *refs):
    prefix_refs, out_ref = refs[:-1], refs[-1]
    paths = pick_ref.shape[1]
    factor = factor_ref[...].astype(jnp.float32)
    for block, sources in enumerate(pieces):
        rows = jnp.concatenate(
            [prefix_refs[k][pl.ds(first, count), :] for k, first, count in sources], axis=0
        )
        picked = lax.dot_general(
            rows, pick_ref[...], (((0,), (0,)), ((), ())), preferred_element_type=jnp.float32
        )
        out_ref[:, pl.ds(block * paths, paths)] = (picked * factor).astype(jnp.bfloat16)


def right_own_kernel(layer_ref, projected_ref, out_ref):
    out_ref[...] = jnp.dot(
        layer_ref[...], projected_ref[...], preferred_element_type=jnp.float32
    ).astype(jnp.bfloat16)


def right_far_kernel(pieces, layer_ref, far_ref, here_ref, *refs):
    (both_ref, near_ref, there_ref), sources = refs[-3:], refs[:-3]
    project_kernel(pieces, *sources, there_ref)
    share = far_ref.shape[0]
    half = near_ref.shape[0] - share
    start = pl.multiple_of(lax.axis_index("tile") * half, half)
    far = far_ref[...]
    both_ref[pl.ds(0, share), :] = jnp.dot(
        far, here_ref[...], preferred_element_type=jnp.float32
    ).astype(jnp.bfloat16)
    cross = jnp.dot(far, there_ref[...], preferred_element_type=jnp.float32).astype(jnp.bfloat16)
    both_ref[pl.ds(share, share), :] = cross
    near_ref[pl.ds(half, share), :] = cross
    near_ref[pl.ds(0, half), :] = jnp.dot(
        layer_ref[pl.ds(start, half), :], there_ref[...], preferred_element_type=jnp.float32
    ).astype(jnp.bfloat16)


def mix_kernel(both_ref, both_t_ref, out_ref):
    share = out_ref.shape[0] // 2
    first = pl.multiple_of(lax.axis_index("tile") * share, share)
    out_ref[pl.ds(0, share), :] = both_ref[pl.ds(first, share), :]
    out_ref[pl.ds(share, share), :] = both_t_ref[pl.ds(first, share), :]


def left_kernel(own_ref, x_ref, projected_ref, mine_ref, other_ref):
    rows, paths = own_ref.shape[0], mine_ref.shape[1]
    for k, layer_ref in enumerate((own_ref, x_ref)):
        states = jnp.dot(
            layer_ref[...], projected_ref[...], preferred_element_type=jnp.float32
        ).astype(jnp.bfloat16)
        mine_ref[pl.ds(k * rows, rows), :] = states[:, :paths]
        other_ref[pl.ds(k * rows, rows), :] = states[:, paths:]


def left_blocks(left_refs):
    for tile, ref in enumerate(left_refs):
        rows = ref.shape[0] // 2
        for half in range(2):
            spin = half * lax.axis_size("tile") + tile
            row = pl.multiple_of((spot_of() ^ spin) * rows, rows)
            yield ref[pl.ds(half * rows, rows), :], rows, row


def amplitude_near_kernel(left_count, *refs):
    left_refs, (own_ref, z_ref, out_ref, right_ref) = refs[:left_count], refs[left_count:]
    chunk = own_ref.shape[0]
    side = right_ref.shape[0] - chunk
    right_ref[pl.ds(0, chunk), :] = own_ref[...]
    right_ref[pl.ds(chunk, side), :] = z_ref[pl.ds(0, side), :]
    right = right_ref[...]
    for left, rows, row in left_blocks(left_refs):
        out_ref[pl.ds(row, rows), :] = lax.dot_general(
            left, right, CONTRACT_LAST, preferred_element_type=jnp.float32
        ).astype(jnp.bfloat16)


def amplitude_rest_kernel(left_count, near_ref, *refs):
    left_refs, right_refs = refs[:left_count], refs[left_count:-4]
    out_ref, right_ref, block_ref, sems = refs[-4:]
    both_ref, mixed_ref, z_ref, both_t_ref, mixed_t_ref, z_t_ref = right_refs
    path, half, tile = (lax.axis_index(axis) for axis in DEVICE_AXES)
    share, halves = both_ref.shape[0] // 2, lax.axis_size("half")
    side = z_ref.shape[0] - share
    chunk = side * lax.axis_size("tile")

    def place(ref, first, far, core, column_half):
        start = side + far * chunk + (core * halves + column_half) * share
        right_ref[pl.ds(pl.multiple_of(start, share), share), :] = ref[pl.ds(first, share), :]

    right_ref[pl.ds(0, side), :] = z_t_ref[pl.ds(0, side), :]
    for core, near, mixed, z in (
        (tile, both_ref, mixed_ref, z_ref), (tile ^ 1, both_t_ref, mixed_t_ref, z_t_ref)
    ):
        place(near, 0, 0, core, half)
        place(z, side, 1, core, half)
        place(mixed, 0, core, core, half ^ 1)
        place(mixed, share, core, core ^ 1, half ^ 1)
    copies = []

    def send(source, row, rows, column, width):
        place = pl.ds(row, rows), pl.ds(pl.multiple_of(column, side), width)
        copy = pltpu.make_async_copy(source, out_ref.at[place], sems.at[len(copies)])
        copies.append(copy)
        copy.start()

    height = near_ref.shape[0]
    send(near_ref.at[:, pl.ds(0, chunk)], 0, height, path * chunk, chunk)
    source = near_ref.at[:, pl.ds(chunk, side)]
    send(source, 0, height, (path ^ 1) * chunk + tile * side, side)
    right = right_ref[...]
    for k, (left, rows, row) in enumerate(left_blocks(left_refs)):
        block_ref[k] = lax.dot_general(
            left, right, CONTRACT_LAST, preferred_element_type=jnp.float32
        ).astype(jnp.bfloat16)
        column = (path ^ 1) * chunk + (tile ^ 1) * side
        send(block_ref.at[k, :, pl.ds(0, side)], row, rows, column, side)
        for far in range(2):
            source = block_ref.at[k, :, pl.ds(side + far * chunk, chunk)]
            send(source, row, rows, (path ^ (2 + far)) * chunk, chunk)
    for copy in copies:
        copy.wait()


def exchanged(
    left_prefix, right_prefix, left_layer, right_layer, left_map, right_map, branch_bits, cut_side
):
    sizes = [lax.axis_size(axis) for axis in DEVICE_AXES]

    def exchange(value, plane=0, half=0, tile=0, tile_plane=0):
        pairs = []
        for p in range(sizes[0]):
            for h in range(sizes[1]):
                for t in range(sizes[2]):
                    source = (p * sizes[1] + h) * sizes[2] + t
                    q = p ^ plane ^ (tile_plane * t)
                    target = (q * sizes[1] + (h ^ half)) * sizes[2] + (t ^ tile)
                    pairs.append((source, target))
        return lax.ppermute(value, DEVICE_AXES, pairs)

    paths = left_map.shape[0]
    depth, gates = right_prefix.shape
    chunk = right_layer.shape[0]
    spots = sizes[1] * sizes[2]
    share = chunk // spots

    prefix_x = exchange(right_prefix, half=1)
    small = (cut_side[None, :], branch_bits.T, left_map[None, :], right_map[None, :])
    far_pack, own, left_own, *small = call(
        stage_kernel,
        [(share, gates), (depth, gates), (depth, gates)]
        + [jax.ShapeDtypeStruct(x.shape, x.dtype) for x in small],
        right_layer, right_prefix, left_prefix, *small,
        in_space=pltpu.HBM,
        scratch=(pltpu.SemaphoreType.DMA((7,)),),
    )
    layer_x = exchange(left_layer, half=1)
    far = exchange(far_pack, plane=2)

    def join(sources, *arrays):
        count = sum(source[2] for source in sources)
        kernel = functools.partial(join_kernel, sources)
        return call(kernel, [(count, arrays[0].shape[1])], *arrays)[0]

    pair = join(((0, 0, depth), (1, 0, depth), (2, 0, depth)), own, prefix_x, left_own)
    near = exchange(pair, plane=1)
    pair_t = exchange(pair, tile=1)
    near_t = exchange(near, tile=1)
    left_factor, left_pick, right_factor, right_pick = call(
        mask_kernel,
        [(gates, paths), (sizes[0] * depth, paths), (gates, paths), (spots * depth, paths)],
        *small,
    )
    left_pair = join(((0, 2 * depth, depth), (1, 2 * depth, depth)), pair, near)
    left_far = exchange(left_pair, plane=2)
    left_far_t = exchange(left_far, tile=1)

    def project(sources, factor, pick, *arrays):
        kernel = functools.partial(project_kernel, sources)
        return call(kernel, [(gates, len(sources) * paths)], factor, pick, *arrays)[0]

    here = project(
        (((0, 0, depth), (1, 0, depth), (0, depth, depth), (1, depth, depth)),),
        right_factor, right_pick, pair, pair_t,
    )
    (right_near,) = call(right_own_kernel, [(chunk, paths)], right_layer, here)
    pieces = (((0, 0, depth), (1, 0, depth), (0, depth, depth), (1, depth, depth)),)
    both, for_near = call(
        functools.partial(right_far_kernel, pieces),
        [(2 * share, paths), (chunk // sizes[2] + share, paths)],
        right_layer, far, here, right_factor, right_pick, near, near_t,
        scratch=(pltpu.VMEM((gates, paths), jnp.bfloat16),),
    )
    both_t = exchange(both, tile=1)
    from_z = exchange(for_near, plane=1)
    (mix,) = call(mix_kernel, [(2 * share, paths)], both, both_t)
    mixed = exchange(mix, half=1, tile_plane=1)
    right_pieces = [
        both, mixed, from_z,
        both_t, exchange(mixed, tile=1), exchange(from_z, tile=1),
    ]
    left_projected = project(
        (
            ((0, 0, 2 * depth), (1, 0, 2 * depth)),
            ((2, 2 * depth, depth), (3, 2 * depth, depth), (4, 0, 2 * depth)),
        ),
        left_factor, left_pick, left_pair, left_far, pair_t, near_t, left_far_t,
    )
    rows = left_layer.shape[0]
    left_mine, left_other = call(
        left_kernel, [(2 * rows, paths)] * 2, left_layer, layer_x, left_projected
    )
    left_states = [left_mine, exchange(left_other, tile=1)]
    side = chunk // sizes[2]
    height = spots * rows
    (amplitude,) = call(
        functools.partial(amplitude_near_kernel, len(left_states)),
        [(height, chunk + side)],
        *left_states, right_near, from_z,
        scratch=(pltpu.VMEM((chunk + side, paths), jnp.bfloat16),),
    )
    return call(
        functools.partial(amplitude_rest_kernel, len(left_states)),
        [(height, sizes[0] * chunk)],
        amplitude, *left_states, *right_pieces,
        scratch=(
            pltpu.VMEM((2 * chunk + side, paths), jnp.bfloat16),
            pltpu.VMEM((spots, rows, 2 * chunk + side), jnp.bfloat16),
            pltpu.SemaphoreType.DMA((2 + 3 * spots,)),
        ),
        out_space=pltpu.HBM,
    )[0]


def solution(mesh):
    in_specs = (
        P(("groups", "path"), ("half", "tile")),
        P(("groups", "half", "tile"), "path"),
        P(("groups", "half", "tile"), None),
        P(("groups", "path"), None),
        P("groups"),
        P("groups"),
        P("groups", None),
        P("groups"),
    )
    out_specs = P(("groups", "half", "tile"), "path")
    squares = (mesh.shape["path"], mesh.shape["half"], mesh.shape["tile"]) == (4, 2, 2)

    def on_device(*arrays):
        return (exchanged if squares else gathered)(*arrays)

    return jax.shard_map(
        on_device, mesh=mesh, in_specs=in_specs, out_specs=out_specs, check_vma=False
    )
```
